128 devices in a mesh: row: 16 (over x_hi, z, core), col: 8 (over x_lo, y).
Axes of the slice: x: 4 (x_hi: 2, x_lo: 2; x = x_hi * 2 + x_lo), y: 4, z: 4, core: 2. Of those that a mesh axis runs over, the one named last changes fastest.
Arguments:
- tokens: bfloat16 [65536, 6144], P(('row', 'col')), may hold values from -6 to 6
- grad_out: bfloat16 [65536, 6144], P(('row', 'col')), may hold values from -6 to 6
- w_up: bfloat16 [6144, 512], replicated, may hold values from -0.078125 to 0.078125
- w_down: bfloat16 [512, 6144], replicated, may hold values from -0.0390625 to 0.0390625
Outputs:
- up_grad: float32 [6144, 512], P('row', 'col')
- down_grad: float32 [6144, 512], P('row', 'col')
The draws below stay inside these ranges and needn't reach their ends.
All inputs are finite; a program needn't handle non-finite values.
Results may differ from the reference program's by a relative error of at most 0.0041.
Values may be sent and summed in bfloat16 or wider, within the bound.
A program may use at most 128 MiB of HBM per device.

```python
import math
import jax
import jax.numpy as jnp
from jax import lax

D = 6144
FF = 24576
C = 512
TOK_DEV = 512
TOKENS = 65536
N_ROW = 16
N_COL = 8


def shard_levels(own_key, shape, cuts, least, top_value):
    factor_of, own = 1.0, jax.random.fold_in(own_key, 6)
    for dim, blocks in cuts:
        steps = jnp.exp(jax.random.uniform(jax.random.fold_in(own, dim), (blocks,), jnp.float32, least / len(cuts), top_value / len(cuts)))
        factor_of = factor_of * jnp.repeat(steps, shape[dim] // blocks).reshape([-1 if axis == dim else 1 for axis in range(len(shape))])
    return factor_of


def normal_values(stream_key, dims, spread, most, cuts=(), kind=jnp.bfloat16):
    drawn = jax.random.normal(stream_key, dims, jnp.float32) * spread
    if len(cuts) > 0:
        drawn = shard_levels(stream_key, dims, cuts, -0.22, 0.18) * drawn
    return jnp.clip(drawn, min=-most, max=most).astype(kind)


def setup_inputs(seed: int = 0) -> dict:
    streams_of = jax.random.split(jax.random.key(seed), 5)
    tokens = normal_values(streams_of[0], (TOKENS, D), 1.0, 6.0, ((0, 128),))
    grad_out = normal_values(streams_of[1], (TOKENS, D), 1.0, 6.0, ((0, 128),))
    w_up = normal_values(streams_of[2], (D, C), D ** -0.5, 0.078125)
    w_down = normal_values(streams_of[3], (C, D), FF ** -0.5, 0.0390625)
    return {"tokens": tokens, "grad_out": grad_out, "w_up": w_up, "w_down": w_down}


def gelu_parts(preact):
    cumul = 0.5 * (1.0 + jax.scipy.special.erf(preact / math.sqrt(2.0)))
    density = jnp.exp(-0.5 * preact * preact) / math.sqrt(2.0 * math.pi)
    return (preact * cumul, cumul + preact * density)

def rounded(term):
    levels = term.astype(jnp.bfloat16)
    levels = lax.optimization_barrier(levels)
    return levels.astype(jnp.float32)

def reference(tokens, grad_out, w_up, w_down):

    def one_device(totals, index):
        start = (index * TOK_DEV).astype(jnp.int32)
        own_tok = lax.dynamic_slice_in_dim(tokens, start, TOK_DEV, 0)
        own_grad = lax.dynamic_slice_in_dim(grad_out, start, TOK_DEV, 0)
        preact = jnp.dot(own_tok, w_up, preferred_element_type=jnp.float32)
        act_grad = jnp.dot(own_grad, w_down.T, preferred_element_type=jnp.float32)
        value, slope = gelu_parts(preact)
        act = value.astype(jnp.bfloat16)
        hidden_grad = (act_grad * slope).astype(jnp.bfloat16)
        term_up = jnp.dot(own_tok.T, hidden_grad, preferred_element_type=jnp.float32)
        term_down = jnp.dot(own_grad.T, act, preferred_element_type=jnp.float32)
        return ((totals[0] + rounded(term_up), totals[1] + rounded(term_down)), None)
    zeros = jnp.zeros((D, C), jnp.float32)
    count = N_ROW * N_COL
    (sum_up, sum_down), _ = lax.scan(one_device, (zeros, zeros), jnp.arange(count, dtype=jnp.int32))
    factor = 1.0 / math.sqrt(TOKENS)
    return (sum_up * factor, sum_down * factor)
```

```python
import functools
import math

import jax
import jax.numpy as jnp
from jax import lax
from jax.experimental import pallas as pl
from jax.experimental.pallas import tpu as pltpu
from jax.sharding import PartitionSpec as P

MESH = pl.DeviceIdType.MESH
BF16, F32 = jnp.bfloat16, jnp.float32
ROOT2, ROOT2PI = math.sqrt(2.0), math.sqrt(2.0 * math.pi)
DOWN, UP = 0, 1
TOK, WIDTH, HID = 512, 6144, 512
AHEAD = 3


def remainder(a, n):
    return lax.rem(a, jnp.int32(n))


def kernel(
    factor,
    tok_hbm, grad_hbm, wup_hbm, wdn_hbm,
    up_ref, dn_ref,
    tok, grad, wup, wdn, tok_mate, grad_mate,
    pre, lin, act, act_mate, hid, hid_mate,
    part, own1, far1, got1, send2, own2, far2, got2, send3, got3,
    load_sem, mate_send, mate_recv, out_sem, in_sem,
):
    row, col = lax.axis_index("row"), lax.axis_index("col")
    core = remainder(row, 2)
    at = {
        "x": (row // 8) * 2 + col // 4,
        "y": remainder(col, 4),
        "z": remainder(row // 2, 4),
    }
    mate = (row + 1 - 2 * core, col)

    def peer(axis, shift):
        to = dict(at)
        to[axis] = remainder(at[axis] + shift, 4)
        return ((to["x"] // 2) * 8 + to["z"] * 2 + core, remainder(to["x"], 2) * 4 + to["y"])

    orders = (("x", "y", "z"), ("y", "z", "x"), ("z", "x", "y"))

    barrier = pltpu.get_barrier_semaphore()
    pl.semaphore_signal(barrier, inc=1, device_id=mate, device_id_type=MESH)
    for axis in ("x", "y", "z"):
        for shift in (1, 3, 2):
            pl.semaphore_signal(barrier, inc=1, device_id=peer(axis, shift), device_id_type=MESH)

    def wide(pair, half):
        return pl.ds(pl.multiple_of(pair * 768 + half * 384, 128), 384)

    loads = []
    for pair in range(8):
        loads.append([
            pltpu.make_async_copy(wup_hbm.at[pl.ds(pair * 768, 768), :], wup.at[pair], load_sem.at[pair, 0]),
            pltpu.make_async_copy(tok_hbm.at[:, wide(pair, 0)], tok.at[pair, 0], load_sem.at[pair, 1]),
            pltpu.make_async_copy(tok_hbm.at[:, wide(pair, 1)], tok.at[pair, 1], load_sem.at[pair, 2]),
        ])
    for pair in range(8):
        loads.append([
            pltpu.make_async_copy(grad_hbm.at[:, wide(pair, 0)], grad.at[pair, 0], load_sem.at[8 + pair, 0]),
            pltpu.make_async_copy(grad_hbm.at[:, wide(pair, 1)], grad.at[pair, 1], load_sem.at[8 + pair, 1]),
        ])
    for pair in range(8):
        loads.append([
            pltpu.make_async_copy(wdn_hbm.at[:, pl.ds(pair * 768, 768)], wdn.at[pair], load_sem.at[16 + pair, 0]),
        ])

    def begin(group):
        for copy in loads[group]:
            copy.start()

    def finish(group):
        for copy in loads[group]:
            copy.wait()

    sent = []

    def send(source, target, sem, to):
        copy = pltpu.make_async_remote_copy(
            src_ref=source, dst_ref=target, send_sem=out_sem.at[sem], recv_sem=in_sem.at[sem],
            device_id=to, device_id_type=MESH,
        )
        copy.start()
        sent.append(copy)
        return copy

    def to_mate(source, target, sem):
        copy = pltpu.make_async_remote_copy(
            src_ref=source, dst_ref=target, send_sem=mate_send.at[sem], recv_sem=mate_recv.at[sem],
            device_id=mate, device_id_type=MESH,
        )
        copy.start()
        sent.append(copy)
        return copy

    for group in range(AHEAD):
        begin(group)
    mate_grad = []
    for pair in range(8):
        finish(pair)
        begin(pair + AHEAD)
        block = jnp.concatenate([tok[pair, 0], tok[pair, 1]], axis=1)
        piece = jnp.dot(block, wup[pair], preferred_element_type=F32)
        pre[...] = piece if pair == 0 else pre[...] + piece
        if pair == 1:
            pl.semaphore_wait(barrier, 10)
            for other in range(8):
                mate_grad.append(to_mate(grad_hbm.at[:, wide(other, 1 - core)], grad_mate.at[other], other))
    for group in range(8 + AHEAD, 24):
        begin(group)
    mate_tok = to_mate(tok.at[:, 1 - core], tok_mate, 8)

    def put_turned(target, i, value):
        target[:, :, pl.ds(pl.multiple_of(i * 128, 128), 128)] = value.astype(BF16).T.reshape(8, 64, 128)

    @pl.loop(0, 4)
    def _(i):
        p = pre[pl.ds(pl.multiple_of(i * 128, 128), 128), :]
        put_turned(act, i, p * (0.5 * (1.0 + lax.erf(p / ROOT2))))

    mate_act = to_mate(act, act_mate, 9)

    def term(left, left_mate, right, right_mate, color, shifts):
        first = orders[color][0]
        lanes = pl.ds(color * 128, 128)
        places = [remainder(at[first] + shift, 4) for shift in shifts]
        if color == 0:
            (place,) = places
            pairs = [(place // 2) * 4 + z for z in range(4)]
            rows = [pl.ds(remainder(place, 2) * 4, 4)]
        elif color == 1:
            pairs = list(range(8))
            rows = [pl.ds(lo * 4 + place, 1) for place in places for lo in range(2)]
        else:
            (place,) = places
            pairs = [place, 4 + place]
            rows = [pl.ds(0, 8)]

        def lhs(ref):
            return jnp.concatenate([ref[r].reshape(r.size * 64, TOK) for r in rows], axis=0)

        a = jnp.concatenate([lhs(left), lhs(left_mate)], axis=1)
        b = jnp.concatenate([
            jnp.concatenate([right[p, core, :, lanes] for p in pairs], axis=1),
            jnp.concatenate([right_mate[p, :, lanes] for p in pairs], axis=1),
        ], axis=0)
        out = jnp.dot(a, b, preferred_element_type=F32)
        chunks = []
        for i in range(len(shifts)):
            got = {}
            for second in range(4):
                for third in range(4):
                    if color == 0:
                        r, l = second * 64, third * 128
                    elif color == 1:
                        r, l = i * 128 + (third % 2) * 64, ((third // 2) * 4 + second) * 128
                    else:
                        r, l = ((second % 2) * 4 + third) * 64, (second // 2) * 128
                    got[second * 4 + third] = out[r:r + 64, l:l + 128]
            chunks.append(got)
        return chunks

    operands = {DOWN: (act, act_mate, grad, grad_mate), UP: (hid, hid_mate, tok, tok_mate)}
    pend = {}

    def keep(bucket, color, shift, chunk):
        for i, value in chunk.items():
            if shift == 0:
                own1[bucket, color, i] = value
            else:
                part[bucket, color, shift - 1, i] = value.astype(BF16)

    def sem_at(bucket, color, which):
        return (bucket * 3 + color) * 15 + which

    def start_far(bucket, color):
        (chunk,) = term(*operands[bucket], color, (2,))
        keep(bucket, color, 2, chunk)
        axis = orders[color][0]
        u = (bucket, color)
        pend[u, 0] = send(part.at[bucket, color, 1, pl.ds(0, 8)], far1.at[bucket, color, 0], sem_at(*u, 0), peer(axis, 1))
        pend[u, 1] = send(part.at[bucket, color, 1, pl.ds(8, 8)], far1.at[bucket, color, 1], sem_at(*u, 1), peer(axis, 3))

    def send_near(bucket, color, shift):
        axis = orders[color][0]
        u = (bucket, color)
        if shift == 1:
            pend[u, 2] = send(part.at[bucket, color, 0, pl.ds(8, 8)], got1.at[bucket, color, 0, pl.ds(8, 8)], sem_at(*u, 2), peer(axis, 1))
        else:
            pend[u, 3] = send(part.at[bucket, color, 2, pl.ds(0, 8)], got1.at[bucket, color, 1, pl.ds(0, 8)], sem_at(*u, 3), peer(axis, 3))

    def start_near(bucket, color):
        if color == 1:
            chunks = term(*operands[bucket], color, (1, 3, 0))
        else:
            chunks = [term(*operands[bucket], color, (shift,))[0] for shift in (1, 3)]
        keep(bucket, color, 1, chunks[0])
        send_near(bucket, color, 1)
        keep(bucket, color, 3, chunks[1])
        send_near(bucket, color, 3)
        if color == 1:
            keep(bucket, color, 0, chunks[2])

    def start_own(bucket, color):
        if color != 1:
            keep(bucket, color, 0, term(*operands[bucket], color, (0,))[0])

    def merge1(bucket, color):
        axis = orders[color][0]
        u = (bucket, color)
        pend[u, 0].wait_recv()
        low, high = pl.ds(0, 8), pl.ds(8, 8)
        part[bucket, color, 0, low] = (
            part[bucket, color, 0, low].astype(F32) + far1[bucket, color, 0].astype(F32)
        ).astype(BF16)
        pend[u, 4] = send(part.at[bucket, color, 0, low], got1.at[bucket, color, 0, low], sem_at(*u, 4), peer(axis, 1))
        pend[u, 1].wait_recv()
        part[bucket, color, 2, high] = (
            part[bucket, color, 2, high].astype(F32) + far1[bucket, color, 1].astype(F32)
        ).astype(BF16)
        pend[u, 5] = send(part.at[bucket, color, 2, high], got1.at[bucket, color, 1, high], sem_at(*u, 5), peer(axis, 3))

    def finish1(bucket, color):
        axis = orders[color][1]
        u = (bucket, color)
        for which in (2, 3, 4, 5):
            pend[u, which].wait_recv()

        def total(shift):
            place = pl.ds(remainder(at[axis] + shift, 4) * 4, 4)
            return (
                own1[bucket, color, place]
                + got1[bucket, color, 0, place].astype(F32)
                + got1[bucket, color, 1, place].astype(F32)
            )

        send2[bucket, color, 1] = total(2).astype(BF16)
        pend[u, 6] = send(send2.at[bucket, color, 1, pl.ds(0, 2)], far2.at[bucket, color, 0], sem_at(*u, 6), peer(axis, 1))
        pend[u, 7] = send(send2.at[bucket, color, 1, pl.ds(2, 2)], far2.at[bucket, color, 1], sem_at(*u, 7), peer(axis, 3))
        send2[bucket, color, 0] = total(1).astype(BF16)
        pend[u, 8] = send(send2.at[bucket, color, 0, pl.ds(2, 2)], got2.at[bucket, color, 0, pl.ds(2, 2)], sem_at(*u, 8), peer(axis, 1))
        send2[bucket, color, 2] = total(3).astype(BF16)
        pend[u, 9] = send(send2.at[bucket, color, 2, pl.ds(0, 2)], got2.at[bucket, color, 1, pl.ds(0, 2)], sem_at(*u, 9), peer(axis, 3))
        own2[bucket, color] = total(0)

    def merge2(bucket, color):
        axis = orders[color][1]
        u = (bucket, color)
        pend[u, 6].wait_recv()
        low, high = pl.ds(0, 2), pl.ds(2, 2)
        send2[bucket, color, 0, low] = (
            send2[bucket, color, 0, low].astype(F32) + far2[bucket, color, 0].astype(F32)
        ).astype(BF16)
        pend[u, 10] = send(send2.at[bucket, color, 0, low], got2.at[bucket, color, 0, low], sem_at(*u, 10), peer(axis, 1))
        pend[u, 7].wait_recv()
        send2[bucket, color, 2, high] = (
            send2[bucket, color, 2, high].astype(F32) + far2[bucket, color, 1].astype(F32)
        ).astype(BF16)
        pend[u, 11] = send(send2.at[bucket, color, 2, high], got2.at[bucket, color, 1, high], sem_at(*u, 11), peer(axis, 3))

    def finish2(bucket, color):
        axis = orders[color][2]
        u = (bucket, color)
        for which in (8, 9, 10, 11):
            pend[u, which].wait_recv()
        for shift in (2, 1, 3):
            place = remainder(at[axis] + shift, 4)
            send3[bucket, color, shift - 1] = (
                own2[bucket, color, place]
                + got2[bucket, color, 0, place].astype(F32)
                + got2[bucket, color, 1, place].astype(F32)
            ).astype(BF16)
            pend[u, 11 + shift] = send(
                send3.at[bucket, color, shift - 1], got3.at[bucket, color, shift - 1], sem_at(*u, 11 + shift), peer(axis, shift)
            )

    def finish3(bucket, color):
        axis = orders[color][2]
        u = (bucket, color)
        place = at[axis]
        total = (
            own2[bucket, color, place]
            + got2[bucket, color, 0, place].astype(F32)
            + got2[bucket, color, 1, place].astype(F32)
        )
        for shift in (1, 3, 2):
            pend[u, 11 + shift].wait_recv()
            total = total + got3[bucket, color, shift - 1].astype(F32)
        out = dn_ref if bucket == DOWN else up_ref
        out[:, pl.ds(color * 128, 128)] = total * factor

    colors = (0, 2, 1)

    for pair in range(8):
        finish(8 + pair)
        mate_grad[pair].wait_recv()
    mate_act.wait_recv()
    for color in colors:
        start_far(DOWN, color)
    for color in colors:
        start_near(DOWN, color)
    for color in colors:
        start_own(DOWN, color)

    def linear(pair):
        finish(16 + pair)
        block = jnp.concatenate([grad[pair, 0], grad[pair, 1]], axis=1)
        piece = lax.dot_general(block, wdn[pair], (((1,), (1,)), ((), ())), preferred_element_type=F32)
        lin[...] = piece if pair == 0 else lin[...] + piece

    for pair in range(4):
        linear(pair)
    for color in colors:
        merge1(DOWN, color)
    for pair in range(4, 8):
        linear(pair)

    @pl.loop(0, 4)
    def _(i):
        rows = pl.ds(pl.multiple_of(i * 128, 128), 128)
        p = pre[rows, :]
        slope = 0.5 * (1.0 + lax.erf(p / ROOT2)) + p * (jnp.exp(-0.5 * p * p) / ROOT2PI)
        put_turned(hid, i, lin[rows, :] * slope)

    mate_hid = to_mate(hid, hid_mate, 10)
    mate_tok.wait_recv()
    mate_hid.wait_recv()
    for color in colors:
        start_far(UP, color)
    for color in colors:
        start_near(UP, color)
    for color in colors:
        finish1(DOWN, color)
    for color in colors:
        start_own(UP, color)
    for color in colors:
        merge2(DOWN, color)
    for color in colors:
        merge1(UP, color)
    for color in colors:
        finish2(DOWN, color)
    for color in colors:
        finish3(DOWN, color)
    for color in colors:
        finish1(UP, color)
    for color in colors:
        merge2(UP, color)
    for color in colors:
        finish2(UP, color)
    for color in colors:
        finish3(UP, color)
    for copy in sent:
        copy.wait_send()


def local(tokens, grad_out, w_up, w_down):
    total_tokens = tokens.shape[0] * lax.axis_size("row") * lax.axis_size("col")
    factor = 1.0 / math.sqrt(total_tokens)
    anywhere = pl.BlockSpec(memory_space=pl.ANY)
    inside = pl.BlockSpec(memory_space=pltpu.VMEM)
    shape = jax.ShapeDtypeStruct((64, 384), F32)
    up, down = pl.pallas_call(
        functools.partial(kernel, factor),
        out_shape=(shape, shape),
        in_specs=[anywhere] * 4,
        out_specs=(inside, inside),
        scratch_shapes=[
            pltpu.VMEM((8, 2, TOK, 384), BF16),
            pltpu.VMEM((8, 2, TOK, 384), BF16),
            pltpu.VMEM((8, 768, HID), BF16),
            pltpu.VMEM((8, HID, 768), BF16),
            pltpu.VMEM((8, TOK, 384), BF16),
            pltpu.VMEM((8, TOK, 384), BF16),
            pltpu.VMEM((TOK, HID), F32),
            pltpu.VMEM((TOK, HID), F32),
            pltpu.VMEM((8, 64, TOK), BF16),
            pltpu.VMEM((8, 64, TOK), BF16),
            pltpu.VMEM((8, 64, TOK), BF16),
            pltpu.VMEM((8, 64, TOK), BF16),
            pltpu.VMEM((2, 3, 3, 16, 64, 128), BF16),
            pltpu.VMEM((2, 3, 16, 64, 128), F32),
            pltpu.VMEM((2, 3, 2, 8, 64, 128), BF16),
            pltpu.VMEM((2, 3, 2, 16, 64, 128), BF16),
            pltpu.VMEM((2, 3, 3, 4, 64, 128), BF16),
            pltpu.VMEM((2, 3, 4, 64, 128), F32),
            pltpu.VMEM((2, 3, 2, 2, 64, 128), BF16),
            pltpu.VMEM((2, 3, 2, 4, 64, 128), BF16),
            pltpu.VMEM((2, 3, 3, 64, 128), BF16),
            pltpu.VMEM((2, 3, 3, 64, 128), BF16),
            pltpu.SemaphoreType.DMA((24, 3)),
            pltpu.SemaphoreType.DMA((11,)),
            pltpu.SemaphoreType.DMA((11,)),
            pltpu.SemaphoreType.DMA((90,)),
            pltpu.SemaphoreType.DMA((90,)),
        ],
        compiler_params=pltpu.CompilerParams(
            collective_id=0, has_side_effects=True, vmem_limit_bytes=66_000_000
        ),
    )(tokens, grad_out, w_up, w_down)
    return up.T, down.T


def solution(mesh):
    placed = (P(("row", "col"), None), P(("row", "col"), None), P(), P())
    return jax.shard_map(
        local,
        mesh=mesh,
        in_specs=placed,
        out_specs=(P("row", "col"), P("row", "col")),
        check_vma=False,
    )
```

```python
import math

import jax
import jax.numpy as jnp
from jax import lax
from jax.experimental import pallas as pl
from jax.experimental.pallas import tpu as pltpu
from jax.sharding import PartitionSpec as P

MESH = pl.DeviceIdType.MESH
BF16, F32 = jnp.bfloat16, jnp.float32
ROOT2, ROOT2PI = math.sqrt(2.0), math.sqrt(2.0 * math.pi)
DOWN, UP = 0, 1
TOK, WIDTH, HID = 512, 6144, 512
AHEAD = 3
EARLY = 2


def remainder(a, n):
    return lax.rem(a, jnp.int32(n))


def kernel(
    tok_hbm, grad_hbm, wup_hbm, wdn_hbm,
    up_ref, dn_ref,
    tok, grad, wup, wdn, tok_mate, grad_mate,
    pre, lin, act, act_mate, hid, hid_mate,
    part, own1, far1, got1, send2, own2, got2, send3, own3, got3,
    load_sem, mate_send, mate_recv, out_sem, in_sem,
):
    row, col = lax.axis_index("row"), lax.axis_index("col")
    core = remainder(row, 2)
    at = {
        "x": (row // 8) * 2 + col // 4,
        "y": remainder(col, 4),
        "z": remainder(row // 2, 4),
    }
    mate = (row + 1 - 2 * core, col)

    def peer(axis, shift):
        to = dict(at)
        to[axis] = remainder(at[axis] + shift, 4)
        return ((to["x"] // 2) * 8 + to["z"] * 2 + core, remainder(to["x"], 2) * 4 + to["y"])

    orders = (("x", "y", "z"), ("y", "z", "x"), ("z", "x", "y"))

    barrier = pltpu.get_barrier_semaphore()
    pl.semaphore_signal(barrier, inc=1, device_id=mate, device_id_type=MESH)
    for axis in ("x", "y", "z"):
        for shift in (1, 3, 2):
            pl.semaphore_signal(barrier, inc=1, device_id=peer(axis, shift), device_id_type=MESH)

    top, deep = at["x"] // 2, at["z"]
    places = [(1 - top, 2), (top, 2), (1 - top, 0), (1 - top, 1), (1 - top, 3), (top, 0), (top, 1), (top, 3)]
    needed = [h * 4 + remainder(deep + d, 4) for h, d in places]

    def both(pair):
        return pl.ds(pl.multiple_of(pair * 768, 128), 768)

    def wide(pair, half):
        return pl.ds(pl.multiple_of(pair * 768 + half * 384, 128), 384)

    loads = []
    for pair in range(8):
        loads.append([
            pltpu.make_async_copy(wup_hbm.at[pl.ds(pair * 768, 768), :], wup.at[pair], load_sem.at[pair]),
            pltpu.make_async_copy(tok_hbm.at[:, wide(pair, 0)], tok.at[pair, 0], load_sem.at[8 + pair]),
            pltpu.make_async_copy(tok_hbm.at[:, wide(pair, 1)], tok.at[pair, 1], load_sem.at[8 + pair]),
        ])
    grad_loads = [[
        pltpu.make_async_copy(grad_hbm.at[:, wide(pair, 0)], grad.at[pair, 0], load_sem.at[16 + i]),
        pltpu.make_async_copy(grad_hbm.at[:, wide(pair, 1)], grad.at[pair, 1], load_sem.at[16 + i]),
    ] for i, pair in enumerate(needed)]
    wdn_loads = [[
        pltpu.make_async_copy(wdn_hbm.at[:, both(pair)], wdn.at[pair], load_sem.at[24 + i]),
    ] for i, pair in enumerate(needed)]
    for i in range(EARLY):
        loads += [grad_loads[i], wdn_loads[i]]
    loads += grad_loads[EARLY:] + wdn_loads[EARLY:]

    def begin(group):
        for copy in loads[group]:
            copy.start()

    def finish(ref, sem):
        pltpu.make_async_copy(ref, ref, load_sem.at[sem]).wait()

    sent = []

    def send(source, target, phase, sem, to):
        pltpu.make_async_remote_copy(
            src_ref=source, dst_ref=target, send_sem=out_sem.at[phase], recv_sem=in_sem.at[sem],
            device_id=to, device_id_type=MESH,
        ).start()

    def sem_at(bucket, color, which):
        return (bucket * 3 + color) * 5 + which

    def arrived(ref, bucket, color, which):
        pltpu.make_async_copy(ref, ref, in_sem.at[sem_at(bucket, color, which)]).wait()

    def to_mate(source, target, sem):
        copy = pltpu.make_async_remote_copy(
            src_ref=source, dst_ref=target, send_sem=mate_send.at[sem], recv_sem=mate_recv.at[sem],
            device_id=mate, device_id_type=MESH,
        )
        copy.start()
        sent.append(copy)
        return copy

    mate_grad = []

    def offer(i):
        mate_grad.append(to_mate(grad_hbm.at[:, wide(needed[i], 1 - core)], grad_mate.at[needed[i]], i))

    for group in range(AHEAD):
        begin(group)
    with jax.named_scope("barrier"):
        pl.semaphore_wait(barrier, 10)
    for pair in range(8):
        with jax.named_scope(f"preact{pair}"):
            finish(wup.at[pair], pair)
            finish(tok.at[pair], 8 + pair)
            begin(pair + AHEAD)
            if pair < 6:
                offer(pair)
            block = jnp.concatenate([tok[pair, 0], tok[pair, 1]], axis=1)
            piece = jnp.dot(block, wup[pair], preferred_element_type=F32)
            pre[...] = piece if pair == 0 else pre[...] + piece
    for group in range(8 + AHEAD, 16 + EARLY):
        begin(group)

    def put_turned(target, i, value):
        target[:, :, pl.ds(pl.multiple_of(i * 128, 128), 128)] = value.astype(BF16).T.reshape(8, 64, 128)

    with jax.named_scope("turn_act"):
        @pl.loop(0, 4)
        def _(i):
            p = pre[pl.ds(pl.multiple_of(i * 128, 128), 128), :]
            put_turned(act, i, p * (0.5 * (1.0 + lax.erf(p / ROOT2))))

    mate_act = to_mate(act, act_mate, 9)
    offer(6)
    offer(7)
    mate_tok = to_mate(tok.at[:, 1 - core], tok_mate, 8)

    def term(left, left_mate, right, right_mate, color, shifts):
        first = orders[color][0]
        lanes = pl.ds(color * 128, 128)
        places = [remainder(at[first] + shift, 4) for shift in shifts]
        if color == 0:
            (place,) = places
            pairs = [(place // 2) * 4 + z for z in range(4)]
            rows = [pl.ds(remainder(place, 2) * 4, 4)]
        elif color == 1:
            pairs = list(range(8))
            rows = [pl.ds(lo * 4 + place, 1) for place in places for lo in range(2)]
        else:
            (place,) = places
            pairs = [place, 4 + place]
            rows = [pl.ds(0, 8)]

        def lhs(ref):
            return jnp.concatenate([ref[r].reshape(r.size * 64, TOK) for r in rows], axis=0)

        a = jnp.concatenate([lhs(left), lhs(left_mate)], axis=1)
        b = jnp.concatenate([
            jnp.concatenate([right[p, core, :, lanes] for p in pairs], axis=1),
            jnp.concatenate([right_mate[p, :, lanes] for p in pairs], axis=1),
        ], axis=0)
        out = jnp.dot(a, b, preferred_element_type=F32)
        chunks = []
        for i in range(len(shifts)):
            got = {}
            for second in range(4):
                for third in range(4):
                    if color == 0:
                        r, l = second * 64, third * 128
                    elif color == 1:
                        r, l = i * 128 + (third % 2) * 64, ((third // 2) * 4 + second) * 128
                    else:
                        r, l = ((second % 2) * 4 + third) * 64, (second // 2) * 128
                    got[second * 4 + third] = out[r:r + 64, l:l + 128]
            chunks.append(got)
        return chunks

    operands = {DOWN: (act, act_mate, grad, grad_mate), UP: (hid, hid_mate, tok, tok_mate)}
    pend = {}
    low, high = pl.ds(0, 8), pl.ds(8, 8)

    def keep(bucket, color, shift, chunk):
        for i, value in chunk.items():
            if shift == 0:
                own1[bucket, color, i] = value
            else:
                part[bucket, color, shift - 1, i] = value.astype(BF16)

    def start_far(bucket, *colors):
        chunks = [term(*operands[bucket], color, (2,))[0] for color in colors]
        for color, chunk in zip(colors, chunks):
            keep(bucket, color, 2, chunk)
        for color in colors:
            axis = orders[color][0]
            send(part.at[bucket, color, 1, low], far1.at[bucket, color, 0], 0, sem_at(bucket, color, 0), peer(axis, 1))
            send(part.at[bucket, color, 1, high], far1.at[bucket, color, 1], 0, sem_at(bucket, color, 1), peer(axis, 3))

    def send_next(bucket, color, half):
        send(part.at[bucket, color, 0, half], got1.at[bucket, color, 0, half], 0, sem_at(bucket, color, 2), peer(orders[color][0], 1))

    def send_last(bucket, color, half):
        send(part.at[bucket, color, 2, half], got1.at[bucket, color, 1, half], 0, sem_at(bucket, color, 2), peer(orders[color][0], 3))

    def start_near(bucket, color):
        if color == 1:
            chunks = term(*operands[bucket], color, (1, 3, 0))
        else:
            chunks = [term(*operands[bucket], color, (shift,))[0] for shift in (1, 3)]
        keep(bucket, color, 1, chunks[0])
        send_next(bucket, color, high)
        keep(bucket, color, 3, chunks[1])
        send_last(bucket, color, low)
        if color == 1:
            keep(bucket, color, 0, chunks[2])

    def start_own(bucket, *colors):
        chunks = [term(*operands[bucket], color, (0,))[0] for color in colors]
        for color, chunk in zip(colors, chunks):
            keep(bucket, color, 0, chunk)

    def merge1(bucket, color):
        for side, shift, half, forward in ((0, 1, low, send_next), (1, 3, high, send_last)):
            arrived(far1.at[bucket, color, side], bucket, color, side)
            part[bucket, color, shift - 1, half] = (
                part[bucket, color, shift - 1, half].astype(F32) + far1[bucket, color, side].astype(F32)
            ).astype(BF16)
            forward(bucket, color, half)

    def finish1(bucket, color):
        axis = orders[color][1]
        arrived(got1.at[bucket, color], bucket, color, 2)

        def total(shift):
            place = pl.ds(remainder(at[axis] + shift, 4) * 4, 4)
            return (
                own1[bucket, color, place]
                + got1[bucket, color, 0, place].astype(F32)
                + got1[bucket, color, 1, place].astype(F32)
            )

        for shift in (2, 1, 3):
            send2[bucket, color, shift - 1] = total(shift).astype(BF16)
            send(send2.at[bucket, color, shift - 1], got2.at[bucket, color, shift - 1], 1, sem_at(bucket, color, 3), peer(axis, shift))
        own2[bucket, color] = total(0)

    def finish2(bucket, color):
        axis = orders[color][2]
        arrived(got2.at[bucket, color], bucket, color, 3)

        def total(place):
            value = own2[bucket, color, place]
            for i in range(3):
                value = value + got2[bucket, color, i, place].astype(F32)
            return value

        for shift in (2, 1, 3):
            send3[bucket, color, shift - 1] = total(remainder(at[axis] + shift, 4)).astype(BF16)
            send(send3.at[bucket, color, shift - 1], got3.at[bucket, color, shift - 1], 2, sem_at(bucket, color, 4), peer(axis, shift))
        own3[bucket, color] = total(at[axis])

    def finish3(bucket, color):
        arrived(got3.at[bucket, color], bucket, color, 4)
        value = own3[bucket, color]
        for i in range(3):
            value = value + got3[bucket, color, i].astype(F32)
        out = dn_ref if bucket == DOWN else up_ref
        out[:, pl.ds(color * 128, 128)] = value

    colors = (2, 0, 1)

    def linear(*order):
        for i in order:
            pair = needed[i]
            finish(wdn.at[pair], 24 + i)
            if i < EARLY:
                finish(grad.at[pair], 16 + i)
            block = jnp.concatenate([grad[pair, 0], grad[pair, 1]], axis=1)
            piece = lax.dot_general(block, wdn[pair], (((1,), (1,)), ((), ())), preferred_element_type=F32)
            lin[...] = piece if i == 0 else lin[...] + piece

    def ready_down(*order):
        for i in order:
            if i >= EARLY:
                finish(grad.at[needed[i]], 16 + i)
            mate_grad[i].wait_recv()

    def ready_act():
        mate_act.wait_recv()
        for group in range(16 + EARLY, 24):
            begin(group)

    def turn_hid():
        @pl.loop(0, 4)
        def _(i):
            rows = pl.ds(pl.multiple_of(i * 128, 128), 128)
            p = pre[rows, :]
            slope = 0.5 * (1.0 + lax.erf(p / ROOT2)) + p * (jnp.exp(-0.5 * p * p) / ROOT2PI)
            put_turned(hid, i, lin[rows, :] * slope)

        pend["hid"] = to_mate(hid, hid_mate, 10)

    def ready_up():
        mate_tok.wait_recv()
        pend["hid"].wait_recv()

    def drain():
        for copy in sent:
            copy.wait_send()
        for phase, ref in enumerate((part, send2, send3)):
            pltpu.make_async_copy(ref, ref, out_sem.at[phase]).wait()

    def one(step, bucket, *colors):
        with jax.named_scope(f"{step.__name__}_{'DU'[bucket]}" + "".join(map(str, colors))):
            step(bucket, *colors)

    def each(step, bucket):
        for color in colors:
            one(step, bucket, color)

    def alone(step, *args):
        with jax.named_scope(step.__name__ + "_".join(str(a) for a in args)):
            step(*args)

    for i in range(EARLY):
        alone(linear, i)
    alone(ready_act)
    alone(ready_down, 0, 1, 2, 3, 4)
    one(start_far, DOWN, 2, 0)
    alone(ready_down, 5, 6, 7)
    one(start_far, DOWN, 1)
    each(start_near, DOWN)
    alone(linear, 2, 3, 4, 5, 6, 7)
    each(merge1, DOWN)
    alone(turn_hid)
    one(start_own, DOWN, 2, 0)
    alone(ready_up)
    one(start_far, UP, 2, 0)
    one(start_far, UP, 1)
    each(finish1, DOWN)
    each(start_near, UP)
    one(start_own, UP, 2, 0)
    each(merge1, UP)
    each(finish2, DOWN)
    each(finish1, UP)
    each(finish3, DOWN)
    each(finish2, UP)
    each(finish3, UP)
    alone(drain)


def local(tokens, grad_out, w_up, w_down):
    total_tokens = tokens.shape[0] * lax.axis_size("row") * lax.axis_size("col")
    factor = 1.0 / math.sqrt(total_tokens)
    anywhere = pl.BlockSpec(memory_space=pl.ANY)
    inside = pl.BlockSpec(memory_space=pltpu.VMEM)
    shape = pltpu.VMEM((64, 384), F32)
    up, down = pl.pallas_call(
        kernel,
        out_shape=(shape, shape),
        in_specs=[anywhere] * 4,
        out_specs=(inside, inside),
        scratch_shapes=[
            pltpu.VMEM((8, 2, TOK, 384), BF16),
            pltpu.VMEM((8, 2, TOK, 384), BF16),
            pltpu.VMEM((8, 768, HID), BF16),
            pltpu.VMEM((8, HID, 768), BF16),
            pltpu.VMEM((8, TOK, 384), BF16),
            pltpu.VMEM((8, TOK, 384), BF16),
            pltpu.VMEM((TOK, HID), F32),
            pltpu.VMEM((TOK, HID), F32),
            pltpu.VMEM((8, 64, TOK), BF16),
            pltpu.VMEM((8, 64, TOK), BF16),
            pltpu.VMEM((8, 64, TOK), BF16),
            pltpu.VMEM((8, 64, TOK), BF16),
            pltpu.VMEM((2, 3, 3, 16, 64, 128), BF16),
            pltpu.VMEM((2, 3, 16, 64, 128), F32),
            pltpu.VMEM((2, 3, 2, 8, 64, 128), BF16),
            pltpu.VMEM((2, 3, 2, 16, 64, 128), BF16),
            pltpu.VMEM((2, 3, 3, 4, 64, 128), BF16),
            pltpu.VMEM((2, 3, 4, 64, 128), F32),
            pltpu.VMEM((2, 3, 3, 4, 64, 128), BF16),
            pltpu.VMEM((2, 3, 3, 64, 128), BF16),
            pltpu.VMEM((2, 3, 64, 128), F32),
            pltpu.VMEM((2, 3, 3, 64, 128), BF16),
            pltpu.SemaphoreType.DMA((32,)),
            pltpu.SemaphoreType.DMA((11,)),
            pltpu.SemaphoreType.DMA((11,)),
            pltpu.SemaphoreType.DMA((3,)),
            pltpu.SemaphoreType.DMA((30,)),
        ],
        compiler_params=pltpu.CompilerParams(
            collective_id=0, has_side_effects=True, vmem_limit_bytes=66_000_000
        ),
    )(tokens, grad_out, w_up, w_down)
    return up.T * factor, down.T * factor


def solution(mesh):
    placed = (P(("row", "col"), None), P(("row", "col"), None), P(), P())
    return jax.shard_map(
        local,
        mesh=mesh,
        in_specs=placed,
        out_specs=(P("row", "col"), P("row", "col")),
        check_vma=False,
    )
```

```python
import math

import jax
import jax.numpy as jnp
from jax import lax
from jax.experimental import pallas as pl
from jax.experimental.pallas import tpu as pltpu
from jax.sharding import PartitionSpec as P

MESH = pl.DeviceIdType.MESH
BF16, F32 = jnp.bfloat16, jnp.float32
ROOT2, ROOT2PI = math.sqrt(2.0), math.sqrt(2.0 * math.pi)
DOWN, UP = 0, 1
TOK, WIDTH, HID = 512, 6144, 512
AHEAD = 4


def remainder(a, n):
    return lax.rem(a, jnp.int32(n))


def kernel(
    tok_hbm, grad_hbm, wup_hbm, wdn_hbm,
    up_ref, dn_ref,
    tok, grad, wup, wdn, tok_mate, grad_mate,
    pre, lin, act, act_mate, hid, hid_mate,
    part, own1, far1, got1, send2, own2, got2, send3, own3, got3,
    load_sem, mate_send, mate_recv, out_sem, in_sem,
):
    row, col = lax.axis_index("row"), lax.axis_index("col")
    core = remainder(row, 2)
    at = {
        "x": (row // 8) * 2 + col // 4,
        "y": remainder(col, 4),
        "z": remainder(row // 2, 4),
    }
    mate = (row + 1 - 2 * core, col)

    def peer(axis, shift):
        to = dict(at)
        to[axis] = remainder(at[axis] + shift, 4)
        return ((to["x"] // 2) * 8 + to["z"] * 2 + core, remainder(to["x"], 2) * 4 + to["y"])

    orders = (("x", "y", "z"), ("y", "z", "x"), ("z", "x", "y"))

    barrier = pltpu.get_barrier_semaphore()
    pl.semaphore_signal(barrier, inc=1, device_id=mate, device_id_type=MESH)
    for axis in ("x", "y", "z"):
        for shift in (1, 3, 2):
            pl.semaphore_signal(barrier, inc=1, device_id=peer(axis, shift), device_id_type=MESH)

    top, deep = at["x"] // 2, at["z"]
    places = [(1 - top, 2), (top, 2), (1 - top, 0), (1 - top, 1), (1 - top, 3), (top, 0), (top, 1), (top, 3)]
    needed = [h * 4 + remainder(deep + d, 4) for h, d in places]

    def both(pair):
        return pl.ds(pl.multiple_of(pair * 768, 128), 768)

    def wide(pair, half):
        return pl.ds(pl.multiple_of(pair * 768 + half * 384, 128), 384)

    loads = []
    for pair in range(8):
        loads.append([
            pltpu.make_async_copy(wup_hbm.at[pl.ds(pair * 768, 768), :], wup.at[pair], load_sem.at[pair]),
            pltpu.make_async_copy(tok_hbm.at[:, wide(pair, 0)], tok.at[pair, 0], load_sem.at[8 + pair]),
            pltpu.make_async_copy(tok_hbm.at[:, wide(pair, 1)], tok.at[pair, 1], load_sem.at[8 + pair]),
        ])
    own_loads, other_loads, wdn_loads = [], [], []
    for i, pair in enumerate(needed):
        own_loads.append([pltpu.make_async_copy(grad_hbm.at[:, wide(pair, core)], grad.at[pair, core], load_sem.at[16 + i])])
        other_loads.append([pltpu.make_async_copy(grad_hbm.at[:, wide(pair, 1 - core)], grad.at[pair, 1 - core], load_sem.at[24 + i])])
        wdn_loads.append([pltpu.make_async_copy(wdn_hbm.at[:, both(pair)], wdn.at[pair], load_sem.at[32 + i])])
    loads += own_loads
    for i in range(8):
        loads.append(other_loads[i] + wdn_loads[i])

    def begin(group):
        for copy in loads[group]:
            copy.start()

    def finish(ref, sem):
        pltpu.make_async_copy(ref, ref, load_sem.at[sem]).wait()

    sent = []

    def send(source, target, phase, sem, to):
        pltpu.make_async_remote_copy(
            src_ref=source, dst_ref=target, send_sem=out_sem.at[phase], recv_sem=in_sem.at[sem],
            device_id=to, device_id_type=MESH,
        ).start()

    def sem_at(bucket, color, which):
        return (bucket * 3 + color) * 5 + which

    def arrived(ref, bucket, color, which):
        pltpu.make_async_copy(ref, ref, in_sem.at[sem_at(bucket, color, which)]).wait()

    def to_mate(source, target, sem):
        copy = pltpu.make_async_remote_copy(
            src_ref=source, dst_ref=target, send_sem=mate_send.at[sem], recv_sem=mate_recv.at[sem],
            device_id=mate, device_id_type=MESH,
        )
        copy.start()
        sent.append(copy)
        return copy

    mate_grad = []

    def offer(i):
        mate_grad.append(to_mate(grad_hbm.at[:, wide(needed[i], 1 - core)], grad_mate.at[needed[i]], i))

    for group in range(AHEAD):
        begin(group)
    with jax.named_scope("barrier"):
        pl.semaphore_wait(barrier, 10)
    for pair in range(8):
        with jax.named_scope(f"preact{pair}"):
            finish(wup.at[pair], pair)
            finish(tok.at[pair], 8 + pair)
            begin(pair + AHEAD)
            if pair < 6:
                offer(pair)
            block = jnp.concatenate([tok[pair, 0], tok[pair, 1]], axis=1)
            piece = jnp.dot(block, wup[pair], preferred_element_type=F32)
            pre[...] = piece if pair == 0 else pre[...] + piece
    for group in range(8 + AHEAD, 18):
        begin(group)

    def put_turned(target, i, value):
        target[:, :, pl.ds(pl.multiple_of(i * 128, 128), 128)] = value.astype(BF16).T.reshape(8, 64, 128)

    def halves(source, target, sem, turn):
        copies = []
        for half in range(2):
            @pl.loop(2 * half, 2 * half + 2)
            def _(i):
                turn(i)

            lanes = pl.ds(half * 256, 256)
            copies.append(to_mate(source.at[:, :, lanes], target.at[:, :, lanes], sem + half))
        return copies

    def turn_act(i):
        p = pre[pl.ds(pl.multiple_of(i * 128, 128), 128), :]
        put_turned(act, i, p * (0.5 * (1.0 + lax.erf(p / ROOT2))))

    with jax.named_scope("turn_act"):
        mate_act = halves(act, act_mate, 9, turn_act)
    offer(6)
    offer(7)
    mate_tok = to_mate(tok.at[:, 1 - core], tok_mate, 8)

    def term(left, left_mate, right, right_mate, color, shifts, sides=("own", "mate")):
        first = orders[color][0]
        lanes = pl.ds(color * 128, 128)
        places = [remainder(at[first] + shift, 4) for shift in shifts]
        if color == 0:
            (place,) = places
            pairs = [(place // 2) * 4 + z for z in range(4)]
            rows = [pl.ds(remainder(place, 2) * 4, 4)]
        elif color == 1:
            pairs = list(range(8))
            rows = [pl.ds(lo * 4 + place, 1) for place in places for lo in range(2)]
        else:
            (place,) = places
            pairs = [place, 4 + place]
            rows = [pl.ds(0, 8)]

        def lhs(ref):
            return jnp.concatenate([ref[r].reshape(r.size * 64, TOK) for r in rows], axis=0)

        a, b = [], []
        if "own" in sides:
            a.append(lhs(left))
            b.append(jnp.concatenate([right[p, core, :, lanes] for p in pairs], axis=1))
        if "mate" in sides:
            a.append(lhs(left_mate))
            b.append(jnp.concatenate([right_mate[p, :, lanes] for p in pairs], axis=1))
        out = jnp.dot(jnp.concatenate(a, axis=1), jnp.concatenate(b, axis=0), preferred_element_type=F32)
        chunks = []
        for i in range(len(shifts)):
            got = {}
            for second in range(4):
                for third in range(4):
                    if color == 0:
                        r, l = second * 64, third * 128
                    elif color == 1:
                        r, l = i * 128 + (third % 2) * 64, ((third // 2) * 4 + second) * 128
                    else:
                        r, l = ((second % 2) * 4 + third) * 64, (second // 2) * 128
                    got[second * 4 + third] = out[r:r + 64, l:l + 128]
            chunks.append(got)
        return chunks

    operands = {DOWN: (act, act_mate, grad, grad_mate), UP: (hid, hid_mate, tok, tok_mate)}
    low, high = pl.ds(0, 8), pl.ds(8, 8)

    def keep(bucket, color, shift, chunk):
        for i, value in chunk.items():
            if shift == 0:
                own1[bucket, color, i] = value
            else:
                part[bucket, color, shift - 1, i] = value.astype(BF16)

    def early_far(bucket, *colors):
        chunks = [term(*operands[bucket], color, (2,), ("own",))[0] for color in colors]
        for color, chunk in zip(colors, chunks):
            keep(bucket, color, 0, chunk)

    def start_far(bucket, *colors):
        chunks = [term(*operands[bucket], color, (2,), ("mate",))[0] for color in colors]
        for color, chunk in zip(colors, chunks):
            keep(bucket, color, 2, {i: value + own1[bucket, color, i] for i, value in chunk.items()})
        for color in colors:
            axis = orders[color][0]
            send(part.at[bucket, color, 1, low], far1.at[bucket, color, 0], 0, sem_at(bucket, color, 0), peer(axis, 1))
            send(part.at[bucket, color, 1, high], far1.at[bucket, color, 1], 0, sem_at(bucket, color, 1), peer(axis, 3))

    def send_next(bucket, color, half, phase=0):
        send(part.at[bucket, color, 0, half], got1.at[bucket, color, 0, half], phase, sem_at(bucket, color, 2), peer(orders[color][0], 1))

    def send_last(bucket, color, half, phase=0):
        send(part.at[bucket, color, 2, half], got1.at[bucket, color, 1, half], phase, sem_at(bucket, color, 2), peer(orders[color][0], 3))

    def start_near(bucket, color):
        if color == 1:
            chunks = term(*operands[bucket], color, (1, 3))
        else:
            chunks = [term(*operands[bucket], color, (shift,))[0] for shift in (1, 3)]
        keep(bucket, color, 1, chunks[0])
        send_next(bucket, color, high)
        keep(bucket, color, 3, chunks[1])
        send_last(bucket, color, low)

    def start_own(bucket, *colors):
        chunks = [term(*operands[bucket], color, (0,))[0] for color in colors]
        for color, chunk in zip(colors, chunks):
            keep(bucket, color, 0, chunk)

    def merge1(bucket, color):
        for side, shift, half, forward in ((0, 1, low, send_next), (1, 3, high, send_last)):
            arrived(far1.at[bucket, color, side], bucket, color, side)
            part[bucket, color, shift - 1, half] = (
                part[bucket, color, shift - 1, half].astype(F32) + far1[bucket, color, side].astype(F32)
            ).astype(BF16)
            forward(bucket, color, half, 3 + bucket * 3 + color)

    def merged(bucket, color):
        pltpu.make_async_copy(part.at[bucket, color, 0], part.at[bucket, color, 0], out_sem.at[3 + bucket * 3 + color]).wait()

    def finish1(bucket, color):
        axis = orders[color][1]
        arrived(got1.at[bucket, color], bucket, color, 2)

        def total(shift):
            place = pl.ds(remainder(at[axis] + shift, 4) * 4, 4)
            return (
                own1[bucket, color, place]
                + got1[bucket, color, 0, place].astype(F32)
                + got1[bucket, color, 1, place].astype(F32)
            )

        for shift in (2, 1, 3):
            send2[bucket, color, shift - 1] = total(shift).astype(BF16)
            send(send2.at[bucket, color, shift - 1], got2.at[bucket, color, shift - 1], 1, sem_at(bucket, color, 3), peer(axis, shift))
        own2[bucket, color] = total(0)

    def finish2(bucket, color):
        axis = orders[color][2]
        arrived(got2.at[bucket, color], bucket, color, 3)

        def total(place):
            value = own2[bucket, color, place]
            for i in range(3):
                value = value + got2[bucket, color, i, place].astype(F32)
            return value

        for shift in (2, 1, 3):
            send3[bucket, color, shift - 1] = total(remainder(at[axis] + shift, 4)).astype(BF16)
            send(send3.at[bucket, color, shift - 1], got3.at[bucket, color, shift - 1], 2, sem_at(bucket, color, 4), peer(axis, shift))
        own3[bucket, color] = total(at[axis])

    def finish3(bucket, color):
        arrived(got3.at[bucket, color], bucket, color, 4)
        value = own3[bucket, color]
        for i in range(3):
            value = value + got3[bucket, color, i].astype(F32)
        out = dn_ref if bucket == DOWN else up_ref
        out[:, pl.ds(color * 128, 128)] = value

    colors = (2, 0, 1)

    def linear(*order):
        for i in order:
            pair = needed[i]
            finish(grad.at[pair, 1 - core], 24 + i)
            finish(wdn.at[pair], 32 + i)
            block = jnp.concatenate([grad[pair, 0], grad[pair, 1]], axis=1)
            piece = lax.dot_general(block, wdn[pair], (((1,), (1,)), ((), ())), preferred_element_type=F32)
            lin[...] = piece if i == 0 else lin[...] + piece

    def ready_grad(*order):
        for i in order:
            finish(grad.at[needed[i], core], 16 + i)

    def ready_mate(*order):
        for i in order:
            mate_grad[i].wait_recv()

    def ready_act():
        for copy in mate_act:
            copy.wait_recv()
        for group in range(18, 24):
            begin(group)

    def turn_hid(i):
        rows = pl.ds(pl.multiple_of(i * 128, 128), 128)
        p = pre[rows, :]
        slope = 0.5 * (1.0 + lax.erf(p / ROOT2)) + p * (jnp.exp(-0.5 * p * p) / ROOT2PI)
        put_turned(hid, i, lin[rows, :] * slope)

    mate_hid = []

    def turn_all_hid():
        mate_hid.extend(halves(hid, hid_mate, 11, turn_hid))

    def ready_up():
        mate_tok.wait_recv()
        for copy in mate_hid:
            copy.wait_recv()

    def drain():
        for copy in sent:
            copy.wait_send()
        for color in colors:
            merged(DOWN, color)
        for phase, ref in enumerate((part.at[:, :, pl.ds(0, 2)], send2, send3)):
            pltpu.make_async_copy(ref, ref, out_sem.at[phase]).wait()

    def one(step, bucket, *colors):
        with jax.named_scope(f"{step.__name__}_{'DU'[bucket]}" + "".join(map(str, colors))):
            step(bucket, *colors)

    def each(step, bucket):
        for color in colors:
            one(step, bucket, color)

    def alone(step, *args):
        with jax.named_scope(step.__name__ + "_".join(str(a) for a in args)):
            step(*args)

    alone(ready_grad, 0, 1, 2, 3, 4)
    one(early_far, DOWN, 2, 0)
    alone(ready_grad, 5, 6, 7)
    one(early_far, DOWN, 1)
    alone(linear, 0)
    alone(ready_act)
    alone(ready_mate, 0, 1, 2, 3, 4)
    one(start_far, DOWN, 2, 0)
    alone(ready_mate, 5, 6, 7)
    one(start_far, DOWN, 1)

    @pl.when(core == 1)
    def _():
        alone(linear, 1)
        alone(linear, 2)
        each(start_near, DOWN)

    @pl.when(core == 0)
    def _():
        each(start_near, DOWN)
        alone(linear, 1)
        alone(linear, 2)
    alone(linear, 3)
    alone(linear, 4)
    alone(linear, 5)
    alone(linear, 6)
    alone(linear, 7)
    each(merge1, DOWN)
    alone(turn_all_hid)
    one(early_far, UP, 2, 0)
    one(early_far, UP, 1)
    one(start_own, DOWN, 2, 0)
    alone(ready_up)
    one(start_far, UP, 2, 0)
    one(start_far, UP, 1)

    @pl.when(core == 1)
    def _():
        one(start_own, DOWN, 1)
        one(start_own, UP, 2, 0, 1)
        each(start_near, UP)

    @pl.when(core == 0)
    def _():
        each(start_near, UP)
        one(start_own, DOWN, 1)
        one(start_own, UP, 2, 0, 1)

    each(merge1, UP)
    for color in colors:
        one(merged, UP, (color + 1) % 3)
        one(finish1, DOWN, color)
    each(finish1, UP)
    each(finish2, DOWN)
    each(finish2, UP)
    each(finish3, DOWN)
    each(finish3, UP)
    alone(drain)


def local(tokens, grad_out, w_up, w_down):
    total_tokens = tokens.shape[0] * lax.axis_size("row") * lax.axis_size("col")
    factor = 1.0 / math.sqrt(total_tokens)
    anywhere = pl.BlockSpec(memory_space=pl.ANY)
    inside = pl.BlockSpec(memory_space=pltpu.VMEM)
    shape = pltpu.VMEM((64, 384), F32)
    up, down = pl.pallas_call(
        kernel,
        out_shape=(shape, shape),
        in_specs=[anywhere] * 4,
        out_specs=(inside, inside),
        scratch_shapes=[
            pltpu.VMEM((8, 2, TOK, 384), BF16),
            pltpu.VMEM((8, 2, TOK, 384), BF16),
            pltpu.VMEM((8, 768, HID), BF16),
            pltpu.VMEM((8, HID, 768), BF16),
            pltpu.VMEM((8, TOK, 384), BF16),
            pltpu.VMEM((8, TOK, 384), BF16),
            pltpu.VMEM((TOK, HID), F32),
            pltpu.VMEM((TOK, HID), F32),
            pltpu.VMEM((8, 64, TOK), BF16),
            pltpu.VMEM((8, 64, TOK), BF16),
            pltpu.VMEM((8, 64, TOK), BF16),
            pltpu.VMEM((8, 64, TOK), BF16),
            pltpu.VMEM((2, 3, 3, 16, 64, 128), BF16),
            pltpu.VMEM((2, 3, 16, 64, 128), F32),
            pltpu.VMEM((2, 3, 2, 8, 64, 128), BF16),
            pltpu.VMEM((2, 3, 2, 16, 64, 128), BF16),
            pltpu.VMEM((2, 3, 3, 4, 64, 128), BF16),
            pltpu.VMEM((2, 3, 4, 64, 128), F32),
            pltpu.VMEM((2, 3, 3, 4, 64, 128), BF16),
            pltpu.VMEM((2, 3, 3, 64, 128), BF16),
            pltpu.VMEM((2, 3, 64, 128), F32),
            pltpu.VMEM((2, 3, 3, 64, 128), BF16),
            pltpu.SemaphoreType.DMA((40,)),
            pltpu.SemaphoreType.DMA((13,)),
            pltpu.SemaphoreType.DMA((13,)),
            pltpu.SemaphoreType.DMA((9,)),
            pltpu.SemaphoreType.DMA((30,)),
        ],
        compiler_params=pltpu.CompilerParams(
            collective_id=0, has_side_effects=True, vmem_limit_bytes=66_000_000
        ),
    )(tokens, grad_out, w_up, w_down)
    return up.T * factor, down.T * factor


def solution(mesh):
    placed = (P(("row", "col"), None), P(("row", "col"), None), P(), P())
    return jax.shard_map(
        local,
        mesh=mesh,
        in_specs=placed,
        out_specs=(P("row", "col"), P("row", "col")),
        check_vma=False,
    )
```

```python
import math

import jax
import jax.numpy as jnp
from jax import lax
from jax.experimental import pallas as pl
from jax.experimental.pallas import tpu as pltpu
from jax.sharding import PartitionSpec as P

MESH = pl.DeviceIdType.MESH
BF16, F32 = jnp.bfloat16, jnp.float32
ROOT2, ROOT2PI = math.sqrt(2.0), math.sqrt(2.0 * math.pi)
DOWN, UP = 0, 1
TOK, WIDTH, HID = 512, 6144, 512
AHEAD = 4
FIRST = 5


def remainder(a, n):
    return lax.rem(a, jnp.int32(n))


def kernel(
    tok_hbm, grad_hbm, wup_hbm, wdn_hbm,
    up_ref, dn_ref,
    tok, grad, wup, wdn, tok_mate, grad_mate,
    pre, lin, act, act_mate, hid, hid_mate,
    part, own1, far1, got1, send2, own2, got2, send3, own3, got3,
    load_sem, mate_send, mate_recv, out_sem, in_sem,
):
    row, col = lax.axis_index("row"), lax.axis_index("col")
    core = remainder(row, 2)
    at = {
        "x": (row // 8) * 2 + col // 4,
        "y": remainder(col, 4),
        "z": remainder(row // 2, 4),
    }
    mate = (row + 1 - 2 * core, col)

    def peer(axis, shift):
        to = dict(at)
        to[axis] = remainder(at[axis] + shift, 4)
        return ((to["x"] // 2) * 8 + to["z"] * 2 + core, remainder(to["x"], 2) * 4 + to["y"])

    orders = (("x", "y", "z"), ("y", "z", "x"), ("z", "x", "y"))

    barrier = pltpu.get_barrier_semaphore()
    pl.semaphore_signal(barrier, inc=1, device_id=mate, device_id_type=MESH)
    for axis in ("x", "y", "z"):
        for shift in (1, 3, 2):
            pl.semaphore_signal(barrier, inc=1, device_id=peer(axis, shift), device_id_type=MESH)

    top, deep = at["x"] // 2, at["z"]
    places = [(1 - top, 2), (top, 2), (1 - top, 0), (1 - top, 1), (1 - top, 3), (top, 0), (top, 1), (top, 3)]
    needed = [h * 4 + remainder(deep + d, 4) for h, d in places]

    def both(pair):
        return pl.ds(pl.multiple_of(pair * 768, 128), 768)

    def wide(pair, half):
        return pl.ds(pl.multiple_of(pair * 768 + half * 384, 128), 384)

    loads = []
    for pair in range(8):
        loads.append([
            pltpu.make_async_copy(wup_hbm.at[pl.ds(pair * 768, 768), :], wup.at[pair], load_sem.at[pair]),
            pltpu.make_async_copy(tok_hbm.at[:, wide(pair, 0)], tok.at[pair, 0], load_sem.at[pair]),
            pltpu.make_async_copy(tok_hbm.at[:, wide(pair, 1)], tok.at[pair, 1], load_sem.at[pair]),
        ])
    own_loads, other_loads = [], []
    for i, pair in enumerate(needed):
        own_loads.append([
            pltpu.make_async_copy(grad_hbm.at[:, wide(pair, core)], grad.at[pair, core], load_sem.at[16 if i < FIRST else 17]),
        ])
        other_loads.append([
            pltpu.make_async_copy(grad_hbm.at[:, wide(pair, 1 - core)], grad.at[pair, 1 - core], load_sem.at[8 + i]),
            pltpu.make_async_copy(wdn_hbm.at[:, both(pair)], wdn.at[pair], load_sem.at[8 + i]),
        ])
    loads += own_loads + other_loads

    def begin(group):
        for copy in loads[group]:
            copy.start()

    def finish(count, sem):
        ref = tok_mate.at[pl.ds(0, count)]
        pltpu.make_async_copy(ref, ref, sem).wait()

    def send(source, target, phase, sem, to):
        pltpu.make_async_remote_copy(
            src_ref=source, dst_ref=target, send_sem=out_sem.at[phase], recv_sem=in_sem.at[sem],
            device_id=to, device_id_type=MESH,
        ).start()

    def sem_at(bucket, color, which):
        return (bucket * 3 + color) * 4 + which

    def arrived(ref, bucket, color, which):
        pltpu.make_async_copy(ref, ref, in_sem.at[sem_at(bucket, color, which)]).wait()

    def to_mate(source, target, out, landed):
        pltpu.make_async_remote_copy(
            src_ref=source, dst_ref=target, send_sem=mate_send.at[out], recv_sem=mate_recv.at[landed],
            device_id=mate, device_id_type=MESH,
        ).start()


    def offer(i):
        to_mate(grad_hbm.at[:, wide(needed[i], 1 - core)], grad_mate.at[needed[i]], 0, 0 if i < FIRST else 1)

    for group in range(AHEAD):
        begin(group)
    with jax.named_scope("barrier"):
        pl.semaphore_wait(barrier, 10)
    def turn(target, i, value):
        target[:, :, pl.ds(i * 128, 128)] = value.astype(BF16).T.reshape(8, 64, 128)

    def turn_act(i):
        p = pre[pl.ds(i * 128, 128), :]
        turn(act, i, p * (0.5 * (1.0 + lax.erf(p / ROOT2))))

    def turn_hid(i):
        rows = pl.ds(i * 128, 128)
        turn(hid, i, lin[rows, :] * pre[rows, :])

    def in_halves(total, product, turned, source, target, out, landed):
        upper, lower = pl.ds(0, 256), pl.ds(256, 256)
        total[upper, :] += product(slice(0, 256))
        piece = product(slice(256, 512))
        turned(0)
        turned(1)
        total[lower, :] += piece
        to_mate(source.at[:, :, upper], target.at[:, :, upper], out, landed)
        turned(2)
        turned(3)
        to_mate(source.at[:, :, lower], target.at[:, :, lower], out, landed)

    for pair in range(8):
        with jax.named_scope(f"preact{pair}"):
            finish(4, load_sem.at[pair])
            begin(pair + AHEAD)
            if pair < 6:
                offer(pair)
            block = jnp.concatenate([tok[pair, 0], tok[pair, 1]], axis=1)
            if pair < 7:
                piece = jnp.dot(block, wup[pair], preferred_element_type=F32)
                pre[...] = piece if pair == 0 else pre[...] + piece
            else:
                for group in range(8 + AHEAD, 18):
                    begin(group)
                in_halves(
                    pre, lambda rows: jnp.dot(block[rows], wup[7], preferred_element_type=F32), turn_act, act, act_mate, 1, 2
                )
    offer(6)
    offer(7)
    to_mate(tok.at[:, 1 - core], tok_mate, 2, 3)

    with jax.named_scope("slope"):
        @pl.loop(0, 4)
        def _(i):
            rows = pl.ds(pl.multiple_of(i * 128, 128), 128)
            p = pre[rows, :]
            pre[rows, :] = 0.5 * (1.0 + lax.erf(p / ROOT2)) + p * (jnp.exp(-0.5 * p * p) / ROOT2PI)

    def term(left, left_mate, right, right_mate, color, shifts, sides=("own", "mate")):
        first = orders[color][0]
        lanes = pl.ds(color * 128, 128)
        places = [remainder(at[first] + shift, 4) for shift in shifts]
        if color == 0:
            (place,) = places
            pairs = [(place // 2) * 4 + z for z in range(4)]
            rows = [pl.ds(remainder(place, 2) * 4, 4)]
        elif color == 1:
            pairs = list(range(8))
            rows = [pl.ds(lo * 4 + place, 1) for place in places for lo in range(2)]
        else:
            (place,) = places
            pairs = [place, 4 + place]
            rows = [pl.ds(0, 8)]

        def lhs(ref):
            return jnp.concatenate([ref[r].reshape(r.size * 64, TOK) for r in rows], axis=0)

        a, b = [], []
        if "own" in sides:
            a.append(lhs(left))
            b.append(jnp.concatenate([right[p, core, :, lanes] for p in pairs], axis=1))
        if "mate" in sides:
            a.append(lhs(left_mate))
            b.append(jnp.concatenate([right_mate[p, :, lanes] for p in pairs], axis=1))
        out = jnp.dot(jnp.concatenate(a, axis=1), jnp.concatenate(b, axis=0), preferred_element_type=F32)
        chunks = []
        for i in range(len(shifts)):
            got = {}
            for second in range(4):
                for third in range(4):
                    if color == 0:
                        r, l = second * 64, third * 128
                    elif color == 1:
                        r, l = i * 128 + (third % 2) * 64, ((third // 2) * 4 + second) * 128
                    else:
                        r, l = ((second % 2) * 4 + third) * 64, (second // 2) * 128
                    got[second * 4 + third] = out[r:r + 64, l:l + 128]
            chunks.append(got)
        return chunks

    operands = {DOWN: (act, act_mate, grad, grad_mate), UP: (hid, hid_mate, tok, tok_mate)}
    low, high = pl.ds(0, 8), pl.ds(8, 8)

    def keep(bucket, color, shift, chunk):
        for i, value in chunk.items():
            if shift == 0:
                own1[bucket, color, i] = value
            else:
                part[bucket, color, shift - 1, i] = value.astype(BF16)

    def early_far(bucket, *colors):
        chunks = [term(*operands[bucket], color, (2,), ("own",))[0] for color in colors]
        for color, chunk in zip(colors, chunks):
            keep(bucket, color, 0, chunk)

    def start_far(bucket, *colors):
        chunks = [term(*operands[bucket], color, (2,), ("mate",))[0] for color in colors]
        for color, chunk in zip(colors, chunks):
            keep(bucket, color, 2, {i: value + own1[bucket, color, i] for i, value in chunk.items()})
        for color in colors:
            axis = orders[color][0]
            send(part.at[bucket, color, 1, low], far1.at[bucket, color, 0], 0, sem_at(bucket, color, 0), peer(axis, 1))
            send(part.at[bucket, color, 1, high], far1.at[bucket, color, 1], 0, sem_at(bucket, color, 0), peer(axis, 3))

    def send_next(bucket, color, half, phase=0):
        send(part.at[bucket, color, 0, half], got1.at[bucket, color, 0, half], phase, sem_at(bucket, color, 1), peer(orders[color][0], 1))

    def send_last(bucket, color, half, phase=0):
        send(part.at[bucket, color, 2, half], got1.at[bucket, color, 1, half], phase, sem_at(bucket, color, 1), peer(orders[color][0], 3))

    def start_near(bucket, color):
        if color == 1:
            chunks = term(*operands[bucket], color, (1, 3))
        else:
            chunks = [term(*operands[bucket], color, (shift,))[0] for shift in (1, 3)]
        keep(bucket, color, 1, chunks[0])
        send_next(bucket, color, high)
        keep(bucket, color, 3, chunks[1])
        send_last(bucket, color, low)

    def start_own(bucket, *colors):
        chunks = [term(*operands[bucket], color, (0,))[0] for color in colors]
        for color, chunk in zip(colors, chunks):
            keep(bucket, color, 0, chunk)

    def merge1(bucket, color):
        arrived(far1.at[bucket, color], bucket, color, 0)
        for side, shift, half, forward in ((0, 1, low, send_next), (1, 3, high, send_last)):
            part[bucket, color, shift - 1, half] = (
                part[bucket, color, shift - 1, half].astype(F32) + far1[bucket, color, side].astype(F32)
            ).astype(BF16)
            forward(bucket, color, half, 1 if bucket == DOWN else 2 + color)

    def merged(bucket, color):
        pltpu.make_async_copy(part.at[bucket, color, 0], part.at[bucket, color, 0], out_sem.at[2 + color]).wait()

    def finish1(bucket, color):
        axis = orders[color][1]
        arrived(got1.at[bucket, color], bucket, color, 1)

        def total(shift):
            place = pl.ds(remainder(at[axis] + shift, 4) * 4, 4)
            return (
                own1[bucket, color, place]
                + got1[bucket, color, 0, place].astype(F32)
                + got1[bucket, color, 1, place].astype(F32)
            )

        for shift in (2, 1, 3):
            send2[bucket, color, shift - 1] = total(shift).astype(BF16)
            send(send2.at[bucket, color, shift - 1], got2.at[bucket, color, shift - 1], 5, sem_at(bucket, color, 2), peer(axis, shift))
        own2[bucket, color] = total(0)

    def finish2(bucket, color):
        axis = orders[color][2]
        arrived(got2.at[bucket, color], bucket, color, 2)

        def total(place):
            value = own2[bucket, color, place]
            for i in range(3):
                value = value + got2[bucket, color, i, place].astype(F32)
            return value

        for shift in (2, 1, 3):
            send3[bucket, color, shift - 1] = total(remainder(at[axis] + shift, 4)).astype(BF16)
            send(send3.at[bucket, color, shift - 1], got3.at[bucket, color, shift - 1], 6, sem_at(bucket, color, 3), peer(axis, shift))
        own3[bucket, color] = total(at[axis])

    def finish3(bucket, color):
        arrived(got3.at[bucket, color], bucket, color, 3)
        value = own3[bucket, color]
        for i in range(3):
            value = value + got3[bucket, color, i].astype(F32)
        out = dn_ref if bucket == DOWN else up_ref
        out[:, pl.ds(color * 128, 128)] = value

    colors = (2, 0, 1)

    def linear(i):
        pair = needed[i]
        finish(3, load_sem.at[8 + i])
        block = jnp.concatenate([grad[pair, 0], grad[pair, 1]], axis=1)

        def product(rows):
            return lax.dot_general(block[rows], wdn[pair], (((1,), (1,)), ((), ())), preferred_element_type=F32)

        if i == 7:
            in_halves(lin, product, turn_hid, hid, hid_mate, 3, 4)
        else:
            piece = product(slice(0, 512))
            lin[...] = piece if i == 0 else lin[...] + piece

    def ready_grad(which):
        finish((FIRST, 8 - FIRST)[which], load_sem.at[16 + which])

    def ready_mate(which):
        finish((FIRST, 8 - FIRST)[which], mate_recv.at[which])

    def ready_act():
        pltpu.make_async_copy(act_mate, act_mate, mate_recv.at[2]).wait()
        for group in range(18, 24):
            begin(group)

    def ready_up():
        pltpu.make_async_copy(tok_mate, tok_mate, mate_recv.at[3]).wait()
        pltpu.make_async_copy(hid_mate, hid_mate, mate_recv.at[4]).wait()

    def drain():
        for i, ref in enumerate((grad_mate, act, tok_mate, hid)):
            pltpu.make_async_copy(ref, ref, mate_send.at[i]).wait()
        for i, ref in ((0, part.at[:, :, pl.ds(0, 2)]), (1, part.at[DOWN, :, 0]), (5, send2), (6, send3)):
            pltpu.make_async_copy(ref, ref, out_sem.at[i]).wait()

    def one(step, bucket, *colors):
        with jax.named_scope(f"{step.__name__}_{'DU'[bucket]}" + "".join(map(str, colors))):
            step(bucket, *colors)

    def each(step, bucket):
        for color in colors:
            one(step, bucket, color)

    def alone(step, *args):
        with jax.named_scope(step.__name__ + "_".join(str(a) for a in args)):
            step(*args)

    alone(ready_grad, 0)
    one(early_far, DOWN, 2, 0)
    alone(ready_grad, 1)
    one(early_far, DOWN, 1)
    alone(linear, 0)
    alone(ready_act)
    alone(ready_mate, 0)
    one(start_far, DOWN, 2, 0)
    alone(ready_mate, 1)
    one(start_far, DOWN, 1)

    @pl.when(core == 1)
    def _():
        alone(linear, 1)
        alone(linear, 2)
        each(start_near, DOWN)

    @pl.when(core == 0)
    def _():
        each(start_near, DOWN)
        alone(linear, 1)
        alone(linear, 2)
    alone(linear, 3)
    alone(linear, 4)
    alone(linear, 5)
    alone(linear, 6)
    alone(linear, 7)
    each(merge1, DOWN)
    one(early_far, UP, 2, 0)
    one(early_far, UP, 1)
    one(start_own, DOWN, 2, 0)
    alone(ready_up)
    one(start_far, UP, 2, 0)
    one(start_far, UP, 1)

    @pl.when(core == 1)
    def _():
        one(start_own, DOWN, 1)
        one(start_own, UP, 2, 0, 1)
        each(start_near, UP)

    @pl.when(core == 0)
    def _():
        each(start_near, UP)
        one(start_own, DOWN, 1)
        one(start_own, UP, 2, 0, 1)

    each(merge1, UP)
    for color in colors:
        one(merged, UP, (color + 1) % 3)
        one(finish1, DOWN, color)
    each(finish1, UP)
    each(finish2, DOWN)
    each(finish2, UP)
    each(finish3, DOWN)
    each(finish3, UP)
    alone(drain)


def local(tokens, grad_out, w_up, w_down):
    total_tokens = tokens.shape[0] * lax.axis_size("row") * lax.axis_size("col")
    factor = 1.0 / math.sqrt(total_tokens)
    anywhere = pl.BlockSpec(memory_space=pl.ANY)
    inside = pl.BlockSpec(memory_space=pltpu.VMEM)
    shape = pltpu.VMEM((64, 384), F32)
    up, down = pl.pallas_call(
        kernel,
        out_shape=(shape, shape),
        in_specs=[anywhere] * 4,
        out_specs=(inside, inside),
        scratch_shapes=[
            pltpu.VMEM((8, 2, TOK, 384), BF16),
            pltpu.VMEM((8, 2, TOK, 384), BF16),
            pltpu.VMEM((8, 768, HID), BF16),
            pltpu.VMEM((8, HID, 768), BF16),
            pltpu.VMEM((8, TOK, 384), BF16),
            pltpu.VMEM((8, TOK, 384), BF16),
            pltpu.VMEM((TOK, HID), F32),
            pltpu.VMEM((TOK, HID), F32),
            pltpu.VMEM((8, 64, TOK), BF16),
            pltpu.VMEM((8, 64, TOK), BF16),
            pltpu.VMEM((8, 64, TOK), BF16),
            pltpu.VMEM((8, 64, TOK), BF16),
            pltpu.VMEM((2, 3, 3, 16, 64, 128), BF16),
            pltpu.VMEM((2, 3, 16, 64, 128), F32),
            pltpu.VMEM((2, 3, 2, 8, 64, 128), BF16),
            pltpu.VMEM((2, 3, 2, 16, 64, 128), BF16),
            pltpu.VMEM((2, 3, 3, 4, 64, 128), BF16),
            pltpu.VMEM((2, 3, 4, 64, 128), F32),
            pltpu.VMEM((2, 3, 3, 4, 64, 128), BF16),
            pltpu.VMEM((2, 3, 3, 64, 128), BF16),
            pltpu.VMEM((2, 3, 64, 128), F32),
            pltpu.VMEM((2, 3, 3, 64, 128), BF16),
            pltpu.SemaphoreType.DMA((18,)),
            pltpu.SemaphoreType.DMA((4,)),
            pltpu.SemaphoreType.DMA((5,)),
            pltpu.SemaphoreType.DMA((7,)),
            pltpu.SemaphoreType.DMA((24,)),
        ],
        compiler_params=pltpu.CompilerParams(
            collective_id=0, has_side_effects=True, vmem_limit_bytes=66_000_000
        ),
    )(tokens, grad_out, w_up, w_down)
    return up.T * factor, down.T * factor


def solution(mesh):
    placed = (P(("row", "col"), None), P(("row", "col"), None), P(), P())
    return jax.shard_map(
        local,
        mesh=mesh,
        in_specs=placed,
        out_specs=(P("row", "col"), P("row", "col")),
        check_vma=False,
    )
```

```python
import math

import jax
import jax.numpy as jnp
from jax import lax
from jax.experimental import pallas as pl
from jax.experimental.pallas import tpu as pltpu
from jax.sharding import PartitionSpec as P

MESH = pl.DeviceIdType.MESH
BF16, F32 = jnp.bfloat16, jnp.float32
ROOT2, ROOT2PI = math.sqrt(2.0), math.sqrt(2.0 * math.pi)
DOWN, UP = 0, 1
TOK, WIDTH, HID = 512, 6144, 512
AHEAD = 4
FIRST = 5


def remainder(a, n):
    return lax.rem(a, jnp.int32(n))


def kernel(
    tok_hbm, grad_hbm, wup_hbm, wdn_hbm,
    up_ref, dn_ref,
    tok, grad, wup, wdn, tok_mate, grad_mate,
    pre, lin, act, act_mate, hid, hid_mate,
    part, own1, far1, got1, send2, own2, far2, got2, send3, own3, got3,
    load_sem, mate_send, mate_recv, out_sem, in_sem,
):
    row, col = lax.axis_index("row"), lax.axis_index("col")
    core = remainder(row, 2)
    at = {
        "x": (row // 8) * 2 + col // 4,
        "y": remainder(col, 4),
        "z": remainder(row // 2, 4),
    }
    mate = (row + 1 - 2 * core, col)

    def peer(axis, shift):
        to = dict(at)
        to[axis] = remainder(at[axis] + shift, 4)
        return ((to["x"] // 2) * 8 + to["z"] * 2 + core, remainder(to["x"], 2) * 4 + to["y"])

    orders = (("x", "y", "z"), ("y", "z", "x"), ("z", "x", "y"))

    barrier = pltpu.get_barrier_semaphore()
    pl.semaphore_signal(barrier, inc=1, device_id=mate, device_id_type=MESH)
    for axis in ("x", "y", "z"):
        for shift in (1, 3, 2):
            pl.semaphore_signal(barrier, inc=1, device_id=peer(axis, shift), device_id_type=MESH)

    top, deep = at["x"] // 2, at["z"]
    places = [(1 - top, 2), (top, 2), (1 - top, 0), (1 - top, 1), (1 - top, 3), (top, 0), (top, 1), (top, 3)]
    needed = [h * 4 + remainder(deep + d, 4) for h, d in places]

    def both(pair):
        return pl.ds(pl.multiple_of(pair * 768, 128), 768)

    def wide(pair, half):
        return pl.ds(pl.multiple_of(pair * 768 + half * 384, 128), 384)

    loads = []
    for pair in range(8):
        loads.append([
            pltpu.make_async_copy(wup_hbm.at[pl.ds(pair * 768, 768), :], wup.at[pair], load_sem.at[pair]),
            pltpu.make_async_copy(tok_hbm.at[:, wide(pair, 0)], tok.at[pair, 0], load_sem.at[pair]),
            pltpu.make_async_copy(tok_hbm.at[:, wide(pair, 1)], tok.at[pair, 1], load_sem.at[pair]),
        ])
    own_loads, other_loads = [], []
    for i, pair in enumerate(needed):
        own_loads.append([
            pltpu.make_async_copy(grad_hbm.at[:, wide(pair, core)], grad.at[pair, core], load_sem.at[16 if i < FIRST else 17]),
        ])
        other_loads.append([
            pltpu.make_async_copy(grad_hbm.at[:, wide(pair, 1 - core)], grad.at[pair, 1 - core], load_sem.at[8 + i]),
            pltpu.make_async_copy(wdn_hbm.at[:, both(pair)], wdn.at[pair], load_sem.at[8 + i]),
        ])
    loads += own_loads + other_loads

    def begin(group):
        for copy in loads[group]:
            copy.start()

    def finish(count, sem):
        ref = tok_mate.at[pl.ds(0, count)]
        pltpu.make_async_copy(ref, ref, sem).wait()

    def send(source, target, phase, sem, to):
        pltpu.make_async_remote_copy(
            src_ref=source, dst_ref=target, send_sem=out_sem.at[phase], recv_sem=in_sem.at[sem],
            device_id=to, device_id_type=MESH,
        ).start()

    def sem_at(bucket, color, which):
        return (bucket * 3 + color) * 4 + which

    def arrived(ref, bucket, color, which):
        pltpu.make_async_copy(ref, ref, in_sem.at[sem_at(bucket, color, which)]).wait()

    def to_mate(source, target, out, landed):
        pltpu.make_async_remote_copy(
            src_ref=source, dst_ref=target, send_sem=mate_send.at[out], recv_sem=mate_recv.at[landed],
            device_id=mate, device_id_type=MESH,
        ).start()


    def offer(i):
        to_mate(grad_hbm.at[:, wide(needed[i], 1 - core)], grad_mate.at[needed[i]], 0, 0 if i < FIRST else 1)

    for group in range(AHEAD):
        begin(group)
    with jax.named_scope("barrier"):
        pl.semaphore_wait(barrier, 10)
    def turn(target, i, value):
        target[:, :, pl.ds(i * 128, 128)] = value.astype(BF16).T.reshape(8, 64, 128)

    def turn_act(i):
        p = pre[pl.ds(i * 128, 128), :]
        turn(act, i, p * (0.5 * (1.0 + lax.erf(p / ROOT2))))

    def turn_hid(i):
        rows = pl.ds(i * 128, 128)
        turn(hid, i, lin[rows, :] * pre[rows, :])

    def in_halves(total, product, turned, source, target, out, landed):
        upper, lower = pl.ds(0, 256), pl.ds(256, 256)
        total[upper, :] += product(slice(0, 256))
        piece = product(slice(256, 512))
        turned(0)
        turned(1)
        total[lower, :] += piece
        to_mate(source.at[:, :, upper], target.at[:, :, upper], out, landed)
        turned(2)
        turned(3)
        to_mate(source.at[:, :, lower], target.at[:, :, lower], out, landed)

    for pair in range(8):
        with jax.named_scope(f"preact{pair}"):
            finish(4, load_sem.at[pair])
            begin(pair + AHEAD)
            if pair < 6:
                offer(pair)
            block = jnp.concatenate([tok[pair, 0], tok[pair, 1]], axis=1)
            if pair < 7:
                piece = jnp.dot(block, wup[pair], preferred_element_type=F32)
                pre[...] = piece if pair == 0 else pre[...] + piece
            else:
                for group in range(8 + AHEAD, 18):
                    begin(group)
                in_halves(
                    pre, lambda rows: jnp.dot(block[rows], wup[7], preferred_element_type=F32), turn_act, act, act_mate, 1, 2
                )
    offer(6)
    offer(7)
    to_mate(tok.at[:, 1 - core], tok_mate, 2, 3)

    with jax.named_scope("slope"):
        @pl.loop(0, 4)
        def _(i):
            rows = pl.ds(pl.multiple_of(i * 128, 128), 128)
            p = pre[rows, :]
            pre[rows, :] = 0.5 * (1.0 + lax.erf(p / ROOT2)) + p * (jnp.exp(-0.5 * p * p) / ROOT2PI)

    def term(left, left_mate, right, right_mate, color, shifts, sides=("own", "mate")):
        first = orders[color][0]
        lanes = pl.ds(color * 128, 128)
        places = [remainder(at[first] + shift, 4) for shift in shifts]
        if color == 0:
            (place,) = places
            pairs = [(place // 2) * 4 + z for z in range(4)]
            rows = [pl.ds(remainder(place, 2) * 4, 4)]
        elif color == 1:
            pairs = list(range(8))
            rows = [pl.ds(lo * 4 + place, 1) for place in places for lo in range(2)]
        else:
            (place,) = places
            pairs = [place, 4 + place]
            rows = [pl.ds(0, 8)]

        def lhs(ref):
            return jnp.concatenate([ref[r].reshape(r.size * 64, TOK) for r in rows], axis=0)

        a, b = [], []
        if "own" in sides:
            a.append(lhs(left))
            b.append(jnp.concatenate([right[p, core, :, lanes] for p in pairs], axis=1))
        if "mate" in sides:
            a.append(lhs(left_mate))
            b.append(jnp.concatenate([right_mate[p, :, lanes] for p in pairs], axis=1))
        out = jnp.dot(jnp.concatenate(a, axis=1), jnp.concatenate(b, axis=0), preferred_element_type=F32)
        chunks = []
        for i in range(len(shifts)):
            got = {}
            for second in range(4):
                for third in range(4):
                    if color == 0:
                        r, l = second * 64, third * 128
                    elif color == 1:
                        r, l = i * 128 + (third % 2) * 64, ((third // 2) * 4 + second) * 128
                    else:
                        r, l = ((second % 2) * 4 + third) * 64, (second // 2) * 128
                    got[second * 4 + third] = out[r:r + 64, l:l + 128]
            chunks.append(got)
        return chunks

    operands = {DOWN: (act, act_mate, grad, grad_mate), UP: (hid, hid_mate, tok, tok_mate)}
    low, high = pl.ds(0, 8), pl.ds(8, 8)
    lower, upper = pl.ds(0, 2), pl.ds(2, 2)

    def keep(bucket, color, shift, chunk):
        for i, value in chunk.items():
            if shift == 0:
                own1[bucket, color, i] = value
            else:
                part[bucket, color, shift - 1, i] = value.astype(BF16)

    def early_far(bucket, *colors):
        chunks = [term(*operands[bucket], color, (2,), ("own",))[0] for color in colors]
        for color, chunk in zip(colors, chunks):
            keep(bucket, color, 0, chunk)

    def start_far(bucket, *colors):
        chunks = [term(*operands[bucket], color, (2,), ("mate",))[0] for color in colors]
        for color, chunk in zip(colors, chunks):
            keep(bucket, color, 2, {i: value + own1[bucket, color, i] for i, value in chunk.items()})
        for color in colors:
            axis = orders[color][0]
            send(part.at[bucket, color, 1, low], far1.at[bucket, color, 0], 0, sem_at(bucket, color, 0), peer(axis, 1))
            send(part.at[bucket, color, 1, high], far1.at[bucket, color, 1], 0, sem_at(bucket, color, 0), peer(axis, 3))

    def send_next(bucket, color, half, phase=0):
        send(part.at[bucket, color, 0, half], got1.at[bucket, color, 0, half], phase, sem_at(bucket, color, 1), peer(orders[color][0], 1))

    def send_last(bucket, color, half, phase=0):
        send(part.at[bucket, color, 2, half], got1.at[bucket, color, 1, half], phase, sem_at(bucket, color, 1), peer(orders[color][0], 3))

    def start_near(bucket, color):
        if color == 1:
            chunks = term(*operands[bucket], color, (1, 3))
        else:
            chunks = [term(*operands[bucket], color, (shift,))[0] for shift in (1, 3)]
        keep(bucket, color, 1, chunks[0])
        send_next(bucket, color, high)
        keep(bucket, color, 3, chunks[1])
        send_last(bucket, color, low)

    def start_own(bucket, *colors):
        chunks = [term(*operands[bucket], color, (0,))[0] for color in colors]
        for color, chunk in zip(colors, chunks):
            keep(bucket, color, 0, chunk)

    def merge1(bucket, color):
        arrived(far1.at[bucket, color], bucket, color, 0)
        for side, shift, half, forward in ((0, 1, low, send_next), (1, 3, high, send_last)):
            part[bucket, color, shift - 1, half] = (
                part[bucket, color, shift - 1, half].astype(F32) + far1[bucket, color, side].astype(F32)
            ).astype(BF16)
            forward(bucket, color, half, 1 if bucket == DOWN else 2 + color)

    def merged(bucket, color):
        pltpu.make_async_copy(part.at[bucket, color, 0], part.at[bucket, color, 0], out_sem.at[2 + color]).wait()

    def total1(bucket, color, shift):
        place = pl.ds(remainder(at[orders[color][1]] + shift, 4) * 4, 4)
        return (
            own1[bucket, color, place]
            + got1[bucket, color, 0, place].astype(F32)
            + got1[bucket, color, 1, place].astype(F32)
        )

    def send_second(bucket, color, source, target, sem, shift):
        send(source, target, 5, sem, peer(orders[color][1], shift))

    def finish1(bucket, color):
        arrived(got1.at[bucket, color], bucket, color, 1)
        sem = sem_at(bucket, color, 2)
        for shift in (2, 1, 3):
            out = send2.at[bucket, color, shift - 1]
            send2[bucket, color, shift - 1] = total1(bucket, color, shift).astype(BF16)
            if bucket == UP:
                send_second(bucket, color, out, got2.at[bucket, color, shift - 1], sem, shift)
            elif shift == 2:
                send_second(bucket, color, out.at[lower], far2.at[color, 0], 24 + color, 1)
                send_second(bucket, color, out.at[upper], far2.at[color, 1], 24 + color, 3)
            elif shift == 1:
                send_second(bucket, color, out.at[upper], got2.at[bucket, color, 0, upper], sem, 1)
            else:
                send_second(bucket, color, out.at[lower], got2.at[bucket, color, 1, lower], sem, 3)
        own2[bucket, color] = total1(bucket, color, 0)

    def merge2(bucket, color):
        pltpu.make_async_copy(far2.at[color], far2.at[color], in_sem.at[24 + color]).wait()
        for side, shift, half in ((0, 1, lower), (1, 3, upper)):
            send2[bucket, color, shift - 1, half] = (
                send2[bucket, color, shift - 1, half].astype(F32) + far2[color, side].astype(F32)
            ).astype(BF16)
            send_second(
                bucket, color, send2.at[bucket, color, shift - 1, half], got2.at[bucket, color, side, half],
                sem_at(bucket, color, 2), shift,
            )

    def finish2(bucket, color):
        axis = orders[color][2]
        count = 2 if bucket == DOWN else 3
        arrived(got2.at[bucket, color, pl.ds(0, count)], bucket, color, 2)

        def total(place):
            value = own2[bucket, color, place]
            for i in range(count):
                value = value + got2[bucket, color, i, place].astype(F32)
            return value

        for shift in (2, 1, 3):
            send3[bucket, color, shift - 1] = total(remainder(at[axis] + shift, 4)).astype(BF16)
            send(send3.at[bucket, color, shift - 1], got3.at[bucket, color, shift - 1], 6, sem_at(bucket, color, 3), peer(axis, shift))
        own3[bucket, color] = total(at[axis])

    def finish3(bucket, color):
        arrived(got3.at[bucket, color], bucket, color, 3)
        value = own3[bucket, color]
        for i in range(3):
            value = value + got3[bucket, color, i].astype(F32)
        out = dn_ref if bucket == DOWN else up_ref
        out[:, pl.ds(color * 128, 128)] = value

    colors = (2, 0, 1)

    def linear(i):
        pair = needed[i]
        finish(3, load_sem.at[8 + i])
        block = jnp.concatenate([grad[pair, 0], grad[pair, 1]], axis=1)

        def product(rows):
            return lax.dot_general(block[rows], wdn[pair], (((1,), (1,)), ((), ())), preferred_element_type=F32)

        if i == 7:
            in_halves(lin, product, turn_hid, hid, hid_mate, 3, 4)
        else:
            piece = product(slice(0, 512))
            lin[...] = piece if i == 0 else lin[...] + piece

    def ready_grad(which):
        finish((FIRST, 8 - FIRST)[which], load_sem.at[16 + which])

    def ready_mate(which):
        finish((FIRST, 8 - FIRST)[which], mate_recv.at[which])

    def ready_act():
        pltpu.make_async_copy(act_mate, act_mate, mate_recv.at[2]).wait()
        for group in range(18, 24):
            begin(group)

    def ready_up():
        pltpu.make_async_copy(tok_mate, tok_mate, mate_recv.at[3]).wait()
        pltpu.make_async_copy(hid_mate, hid_mate, mate_recv.at[4]).wait()

    def drain():
        for i, ref in enumerate((grad_mate, act, tok_mate, hid)):
            pltpu.make_async_copy(ref, ref, mate_send.at[i]).wait()
        for i, ref in ((0, part.at[:, :, pl.ds(0, 2)]), (1, part.at[DOWN, :, 0]), (5, send2), (6, send3)):
            pltpu.make_async_copy(ref, ref, out_sem.at[i]).wait()

    def one(step, bucket, *colors):
        with jax.named_scope(f"{step.__name__}_{'DU'[bucket]}" + "".join(map(str, colors))):
            step(bucket, *colors)

    def each(step, bucket):
        for color in colors:
            one(step, bucket, color)

    def alone(step, *args):
        with jax.named_scope(step.__name__ + "_".join(str(a) for a in args)):
            step(*args)

    alone(ready_grad, 0)
    one(early_far, DOWN, 2, 0)
    alone(ready_grad, 1)
    one(early_far, DOWN, 1)
    alone(linear, 0)
    alone(ready_act)
    alone(ready_mate, 0)
    one(start_far, DOWN, 2, 0)
    alone(ready_mate, 1)
    one(start_far, DOWN, 1)

    @pl.when(core == 1)
    def _():
        alone(linear, 1)
        alone(linear, 2)
        each(start_near, DOWN)

    @pl.when(core == 0)
    def _():
        each(start_near, DOWN)
        alone(linear, 1)
        alone(linear, 2)
    alone(linear, 3)
    alone(linear, 4)
    alone(linear, 5)
    alone(linear, 6)
    alone(linear, 7)
    each(merge1, DOWN)
    one(early_far, UP, 2, 0)
    one(early_far, UP, 1)
    one(start_own, DOWN, 2, 0)
    alone(ready_up)
    one(start_far, UP, 2, 0)
    one(start_far, UP, 1)

    @pl.when(core == 1)
    def _():
        one(start_own, DOWN, 1)
        one(start_own, UP, 2, 0, 1)
        each(start_near, UP)

    @pl.when(core == 0)
    def _():
        each(start_near, UP)
        one(start_own, DOWN, 1)
        one(start_own, UP, 2, 0, 1)

    each(merge1, UP)
    for color in colors:
        one(merged, UP, (color + 1) % 3)
        one(finish1, DOWN, color)
    each(finish1, UP)
    each(merge2, DOWN)
    each(finish2, UP)
    each(finish2, DOWN)
    each(finish3, UP)
    each(finish3, DOWN)
    alone(drain)


def local(tokens, grad_out, w_up, w_down):
    total_tokens = tokens.shape[0] * lax.axis_size("row") * lax.axis_size("col")
    factor = 1.0 / math.sqrt(total_tokens)
    anywhere = pl.BlockSpec(memory_space=pl.ANY)
    inside = pl.BlockSpec(memory_space=pltpu.VMEM)
    shape = pltpu.VMEM((64, 384), F32)
    up, down = pl.pallas_call(
        kernel,
        out_shape=(shape, shape),
        in_specs=[anywhere] * 4,
        out_specs=(inside, inside),
        scratch_shapes=[
            pltpu.VMEM((8, 2, TOK, 384), BF16),
            pltpu.VMEM((8, 2, TOK, 384), BF16),
            pltpu.VMEM((8, 768, HID), BF16),
            pltpu.VMEM((8, HID, 768), BF16),
            pltpu.VMEM((8, TOK, 384), BF16),
            pltpu.VMEM((8, TOK, 384), BF16),
            pltpu.VMEM((TOK, HID), F32),
            pltpu.VMEM((TOK, HID), F32),
            pltpu.VMEM((8, 64, TOK), BF16),
            pltpu.VMEM((8, 64, TOK), BF16),
            pltpu.VMEM((8, 64, TOK), BF16),
            pltpu.VMEM((8, 64, TOK), BF16),
            pltpu.VMEM((2, 3, 3, 16, 64, 128), BF16),
            pltpu.VMEM((2, 3, 16, 64, 128), F32),
            pltpu.VMEM((2, 3, 2, 8, 64, 128), BF16),
            pltpu.VMEM((2, 3, 2, 16, 64, 128), BF16),
            pltpu.VMEM((2, 3, 3, 4, 64, 128), BF16),
            pltpu.VMEM((2, 3, 4, 64, 128), F32),
            pltpu.VMEM((3, 2, 2, 64, 128), BF16),
            pltpu.VMEM((2, 3, 3, 4, 64, 128), BF16),
            pltpu.VMEM((2, 3, 3, 64, 128), BF16),
            pltpu.VMEM((2, 3, 64, 128), F32),
            pltpu.VMEM((2, 3, 3, 64, 128), BF16),
            pltpu.SemaphoreType.DMA((18,)),
            pltpu.SemaphoreType.DMA((4,)),
            pltpu.SemaphoreType.DMA((5,)),
            pltpu.SemaphoreType.DMA((7,)),
            pltpu.SemaphoreType.DMA((27,)),
        ],
        compiler_params=pltpu.CompilerParams(
            collective_id=0, has_side_effects=True, vmem_limit_bytes=66_000_000
        ),
    )(tokens, grad_out, w_up, w_down)
    return up.T * factor, down.T * factor


def solution(mesh):
    placed = (P(("row", "col"), None), P(("row", "col"), None), P(), P())
    return jax.shard_map(
        local,
        mesh=mesh,
        in_specs=placed,
        out_specs=(P("row", "col"), P("row", "col")),
        check_vma=False,
    )
```

```python
import math

import jax
import jax.numpy as jnp
from jax import lax
from jax.experimental import pallas as pl
from jax.experimental.pallas import tpu as pltpu
from jax.sharding import PartitionSpec as P

MESH = pl.DeviceIdType.MESH
BF16, F32 = jnp.bfloat16, jnp.float32
ROOT2, ROOT2PI = math.sqrt(2.0), math.sqrt(2.0 * math.pi)
DOWN, UP = 0, 1
TOK, WIDTH, HID = 512, 6144, 512
AHEAD = 4
FIRST = 5


def remainder(a, n):
    return lax.rem(a, jnp.int32(n))


def kernel(
    tok_hbm, grad_hbm, wup_hbm, wdn_hbm,
    up_ref, dn_ref,
    tok, grad, wup, wdn, tok_mate, grad_mate,
    pre, lin, act, act_mate, hid, hid_mate,
    part, own1, far1, got1, send2, own2, far2, got2, send3, own3, got3,
    load_sem, mate_send, mate_recv, out_sem, in_sem,
):
    row, col = lax.axis_index("row"), lax.axis_index("col")
    core = remainder(row, 2)
    at = {
        "x": (row // 8) * 2 + col // 4,
        "y": remainder(col, 4),
        "z": remainder(row // 2, 4),
    }
    mate = (row + 1 - 2 * core, col)

    def peer(axis, shift):
        to = dict(at)
        to[axis] = remainder(at[axis] + shift, 4)
        return ((to["x"] // 2) * 8 + to["z"] * 2 + core, remainder(to["x"], 2) * 4 + to["y"])

    orders = (("x", "y", "z"), ("y", "z", "x"), ("z", "x", "y"))

    barrier = pltpu.get_barrier_semaphore()
    pl.semaphore_signal(barrier, inc=1, device_id=mate, device_id_type=MESH)
    for axis in ("x", "y", "z"):
        for shift in (1, 3, 2):
            pl.semaphore_signal(barrier, inc=1, device_id=peer(axis, shift), device_id_type=MESH)

    top, deep = at["x"] // 2, at["z"]
    places = [(1 - top, 2), (top, 2), (1 - top, 0), (1 - top, 1), (1 - top, 3), (top, 0), (top, 1), (top, 3)]
    needed = [h * 4 + remainder(deep + d, 4) for h, d in places]

    def both(pair):
        return pl.ds(pl.multiple_of(pair * 768, 128), 768)

    def wide(pair, half):
        return pl.ds(pl.multiple_of(pair * 768 + half * 384, 128), 384)

    loads = []
    for pair in range(8):
        loads.append([
            pltpu.make_async_copy(wup_hbm.at[pl.ds(pair * 768, 768), :], wup.at[pair], load_sem.at[pair]),
            pltpu.make_async_copy(tok_hbm.at[:, wide(pair, 0)], tok.at[pair, 0], load_sem.at[pair]),
            pltpu.make_async_copy(tok_hbm.at[:, wide(pair, 1)], tok.at[pair, 1], load_sem.at[pair]),
        ])
    own_loads, other_loads = [], []
    for i, pair in enumerate(needed):
        own_loads.append([
            pltpu.make_async_copy(grad_hbm.at[:, wide(pair, core)], grad.at[pair, core], load_sem.at[16 if i < FIRST else 17]),
        ])
        other_loads.append([
            pltpu.make_async_copy(grad_hbm.at[:, wide(pair, 1 - core)], grad.at[pair, 1 - core], load_sem.at[8 + i]),
            pltpu.make_async_copy(wdn_hbm.at[:, both(pair)], wdn.at[pair], load_sem.at[8 + i]),
        ])
    loads += own_loads + other_loads

    def begin(group):
        for copy in loads[group]:
            copy.start()

    def finish(count, sem):
        ref = tok_mate.at[pl.ds(0, count)]
        pltpu.make_async_copy(ref, ref, sem).wait()

    def send(source, target, phase, sem, to):
        pltpu.make_async_remote_copy(
            src_ref=source, dst_ref=target, send_sem=out_sem.at[phase], recv_sem=in_sem.at[sem],
            device_id=to, device_id_type=MESH,
        ).start()

    def sem_at(bucket, color, which):
        return (bucket * 3 + color) * 4 + which

    def arrived(ref, bucket, color, which):
        pltpu.make_async_copy(ref, ref, in_sem.at[sem_at(bucket, color, which)]).wait()

    def to_mate(source, target, out, landed):
        pltpu.make_async_remote_copy(
            src_ref=source, dst_ref=target, send_sem=mate_send.at[out], recv_sem=mate_recv.at[landed],
            device_id=mate, device_id_type=MESH,
        ).start()


    def offer(i):
        to_mate(grad_hbm.at[:, wide(needed[i], 1 - core)], grad_mate.at[needed[i]], 0, 0 if i < FIRST else 1)

    for group in range(AHEAD):
        begin(group)
    with jax.named_scope("barrier"):
        pl.semaphore_wait(barrier, 10)
    def turn(target, i, value):
        target[:, :, pl.ds(i * 128, 128)] = value.astype(BF16).T.reshape(8, 64, 128)

    def turn_act(i):
        p = pre[pl.ds(i * 128, 128), :]
        turn(act, i, p * (0.5 * (1.0 + lax.erf(p / ROOT2))))

    def turn_hid(i):
        rows = pl.ds(i * 128, 128)
        turn(hid, i, lin[rows, :] * pre[rows, :])

    def in_halves(total, product, turned, source, target, out, landed):
        upper, lower = pl.ds(0, 256), pl.ds(256, 256)
        total[upper, :] += product(slice(0, 256))
        piece = product(slice(256, 512))
        turned(0)
        turned(1)
        total[lower, :] += piece
        to_mate(source.at[:, :, upper], target.at[:, :, upper], out, landed)
        turned(2)
        turned(3)
        to_mate(source.at[:, :, lower], target.at[:, :, lower], out, landed)

    for pair in range(8):
        with jax.named_scope(f"preact{pair}"):
            finish(4, load_sem.at[pair])
            begin(pair + AHEAD)
            if pair < 6:
                offer(pair)
            block = jnp.concatenate([tok[pair, 0], tok[pair, 1]], axis=1)
            if pair < 7:
                piece = jnp.dot(block, wup[pair], preferred_element_type=F32)
                pre[...] = piece if pair == 0 else pre[...] + piece
            else:
                for group in range(8 + AHEAD, 18):
                    begin(group)
                in_halves(
                    pre, lambda rows: jnp.dot(block[rows], wup[7], preferred_element_type=F32), turn_act, act, act_mate, 1, 2
                )
    offer(6)
    offer(7)
    to_mate(tok.at[:, 1 - core], tok_mate, 2, 3)

    with jax.named_scope("slope"):
        @pl.loop(0, 4)
        def _(i):
            rows = pl.ds(pl.multiple_of(i * 128, 128), 128)
            p = pre[rows, :]
            pre[rows, :] = 0.5 * (1.0 + lax.erf(p / ROOT2)) + p * (jnp.exp(-0.5 * p * p) / ROOT2PI)

    def term(left, left_mate, right, right_mate, color, shifts, sides=("own", "mate")):
        first = orders[color][0]
        lanes = pl.ds(color * 128, 128)
        places = [remainder(at[first] + shift, 4) for shift in shifts]
        if color == 0:
            (place,) = places
            pairs = [(place // 2) * 4 + z for z in range(4)]
            rows = [pl.ds(remainder(place, 2) * 4, 4)]
        elif color == 1:
            pairs = list(range(8))
            rows = [pl.ds(lo * 4 + place, 1) for place in places for lo in range(2)]
        else:
            (place,) = places
            pairs = [place, 4 + place]
            rows = [pl.ds(0, 8)]

        def lhs(ref):
            return jnp.concatenate([ref[r].reshape(r.size * 64, TOK) for r in rows], axis=0)

        a, b = [], []
        if "own" in sides:
            a.append(lhs(left))
            b.append(jnp.concatenate([right[p, core, :, lanes] for p in pairs], axis=1))
        if "mate" in sides:
            a.append(lhs(left_mate))
            b.append(jnp.concatenate([right_mate[p, :, lanes] for p in pairs], axis=1))
        out = jnp.dot(jnp.concatenate(a, axis=1), jnp.concatenate(b, axis=0), preferred_element_type=F32)
        chunks = []
        for i in range(len(shifts)):
            got = {}
            for second in range(4):
                for third in range(4):
                    if color == 0:
                        r, l = second * 64, third * 128
                    elif color == 1:
                        r, l = i * 128 + (third % 2) * 64, ((third // 2) * 4 + second) * 128
                    else:
                        r, l = ((second % 2) * 4 + third) * 64, (second // 2) * 128
                    got[second * 4 + third] = out[r:r + 64, l:l + 128]
            chunks.append(got)
        return chunks

    operands = {DOWN: (act, act_mate, grad, grad_mate), UP: (hid, hid_mate, tok, tok_mate)}
    low, high = pl.ds(0, 8), pl.ds(8, 8)
    lower, upper = pl.ds(0, 2), pl.ds(2, 2)

    def keep(bucket, color, shift, chunk):
        for i, value in chunk.items():
            if shift == 0:
                own1[bucket, color, i] = value
            else:
                part[bucket, color, shift - 1, i] = value.astype(BF16)

    def early_far(bucket, *colors):
        chunks = [term(*operands[bucket], color, (2,), ("own",))[0] for color in colors]
        for color, chunk in zip(colors, chunks):
            keep(bucket, color, 0, chunk)

    def whole_far(bucket, *colors):
        chunks = [term(*operands[bucket], color, (2,))[0] for color in colors]
        for color, chunk in zip(colors, chunks):
            keep(bucket, color, 2, chunk)
        send_far(bucket, *colors)

    def start_far(bucket, *colors):
        chunks = [term(*operands[bucket], color, (2,), ("mate",))[0] for color in colors]
        for color, chunk in zip(colors, chunks):
            keep(bucket, color, 2, {i: value + own1[bucket, color, i] for i, value in chunk.items()})
        send_far(bucket, *colors)

    def send_far(bucket, *colors):
        for color in colors:
            axis = orders[color][0]
            send(part.at[bucket, color, 1, low], far1.at[bucket, color, 0], 0, sem_at(bucket, color, 0), peer(axis, 1))
            send(part.at[bucket, color, 1, high], far1.at[bucket, color, 1], 0, sem_at(bucket, color, 0), peer(axis, 3))

    def send_next(bucket, color, half, phase=0):
        send(part.at[bucket, color, 0, half], got1.at[bucket, color, 0, half], phase, sem_at(bucket, color, 1), peer(orders[color][0], 1))

    def send_last(bucket, color, half, phase=0):
        send(part.at[bucket, color, 2, half], got1.at[bucket, color, 1, half], phase, sem_at(bucket, color, 1), peer(orders[color][0], 3))

    def start_near(bucket, color):
        if color == 1:
            chunks = term(*operands[bucket], color, (1, 3))
        else:
            chunks = [term(*operands[bucket], color, (shift,))[0] for shift in (1, 3)]
        keep(bucket, color, 1, chunks[0])
        send_next(bucket, color, high)
        keep(bucket, color, 3, chunks[1])
        send_last(bucket, color, low)

    def start_own(bucket, *colors):
        chunks = [term(*operands[bucket], color, (0,))[0] for color in colors]
        for color, chunk in zip(colors, chunks):
            keep(bucket, color, 0, chunk)

    def merge1(bucket, color):
        arrived(far1.at[bucket, color], bucket, color, 0)
        for side, shift, half, forward in ((0, 1, low, send_next), (1, 3, high, send_last)):
            part[bucket, color, shift - 1, half] = (
                part[bucket, color, shift - 1, half].astype(F32) + far1[bucket, color, side].astype(F32)
            ).astype(BF16)
            forward(bucket, color, half, 1 if bucket == DOWN else 2 + color)

    def merged(bucket, color):
        pltpu.make_async_copy(part.at[bucket, color, 0], part.at[bucket, color, 0], out_sem.at[2 + color]).wait()

    def total1(bucket, color, shift):
        place = pl.ds(remainder(at[orders[color][1]] + shift, 4) * 4, 4)
        return (
            own1[bucket, color, place]
            + got1[bucket, color, 0, place].astype(F32)
            + got1[bucket, color, 1, place].astype(F32)
        )

    def send_second(bucket, color, source, target, sem, shift):
        send(source, target, 5, sem, peer(orders[color][1], shift))

    def finish1(bucket, color):
        arrived(got1.at[bucket, color], bucket, color, 1)
        sem = sem_at(bucket, color, 2)
        for shift in (2, 1, 3):
            out = send2.at[bucket, color, shift - 1]
            send2[bucket, color, shift - 1] = total1(bucket, color, shift).astype(BF16)
            if bucket == UP:
                send_second(bucket, color, out, got2.at[bucket, color, shift - 1], sem, shift)
            elif shift == 2:
                send_second(bucket, color, out.at[lower], far2.at[color, 0], 24 + color, 1)
                send_second(bucket, color, out.at[upper], far2.at[color, 1], 24 + color, 3)
            elif shift == 1:
                send_second(bucket, color, out.at[upper], got2.at[bucket, color, 0, upper], sem, 1)
            else:
                send_second(bucket, color, out.at[lower], got2.at[bucket, color, 1, lower], sem, 3)
        own2[bucket, color] = total1(bucket, color, 0)

    def merge2(bucket, color):
        pltpu.make_async_copy(far2.at[color], far2.at[color], in_sem.at[24 + color]).wait()
        for side, shift, half in ((0, 1, lower), (1, 3, upper)):
            send2[bucket, color, shift - 1, half] = (
                send2[bucket, color, shift - 1, half].astype(F32) + far2[color, side].astype(F32)
            ).astype(BF16)
            send_second(
                bucket, color, send2.at[bucket, color, shift - 1, half], got2.at[bucket, color, side, half],
                sem_at(bucket, color, 2), shift,
            )

    def finish2(bucket, color):
        axis = orders[color][2]
        count = 2 if bucket == DOWN else 3
        arrived(got2.at[bucket, color, pl.ds(0, count)], bucket, color, 2)

        def total(place):
            value = own2[bucket, color, place]
            for i in range(count):
                value = value + got2[bucket, color, i, place].astype(F32)
            return value

        for shift in (2, 1, 3):
            send3[bucket, color, shift - 1] = total(remainder(at[axis] + shift, 4)).astype(BF16)
            send(send3.at[bucket, color, shift - 1], got3.at[bucket, color, shift - 1], 6, sem_at(bucket, color, 3), peer(axis, shift))
        own3[bucket, color] = total(at[axis])

    def finish3(bucket, color):
        arrived(got3.at[bucket, color], bucket, color, 3)
        value = own3[bucket, color]
        for i in range(3):
            value = value + got3[bucket, color, i].astype(F32)
        out = dn_ref if bucket == DOWN else up_ref
        out[:, pl.ds(color * 128, 128)] = value

    colors = (2, 0, 1)

    def linear(i):
        pair = needed[i]
        finish(3, load_sem.at[8 + i])
        block = jnp.concatenate([grad[pair, 0], grad[pair, 1]], axis=1)

        def product(rows):
            return lax.dot_general(block[rows], wdn[pair], (((1,), (1,)), ((), ())), preferred_element_type=F32)

        if i == 7:
            in_halves(lin, product, turn_hid, hid, hid_mate, 3, 4)
        else:
            piece = product(slice(0, 512))
            lin[...] = piece if i == 0 else lin[...] + piece

    def ready_grad(which):
        finish((FIRST, 8 - FIRST)[which], load_sem.at[16 + which])

    def ready_mate(which):
        finish((FIRST, 8 - FIRST)[which], mate_recv.at[which])

    def ready_act():
        pltpu.make_async_copy(act_mate, act_mate, mate_recv.at[2]).wait()
        for group in range(18, 24):
            begin(group)

    def ready_up():
        pltpu.make_async_copy(tok_mate, tok_mate, mate_recv.at[3]).wait()
        pltpu.make_async_copy(hid_mate, hid_mate, mate_recv.at[4]).wait()

    def drain():
        for i, ref in enumerate((grad_mate, act, tok_mate, hid)):
            pltpu.make_async_copy(ref, ref, mate_send.at[i]).wait()
        for i, ref in ((0, part.at[:, :, pl.ds(0, 2)]), (1, part.at[DOWN, :, 0]), (5, send2), (6, send3)):
            pltpu.make_async_copy(ref, ref, out_sem.at[i]).wait()

    def one(step, bucket, *colors):
        with jax.named_scope(f"{step.__name__}_{'DU'[bucket]}" + "".join(map(str, colors))):
            step(bucket, *colors)

    def each(step, bucket):
        for color in colors:
            one(step, bucket, color)

    def alone(step, *args):
        with jax.named_scope(step.__name__ + "_".join(str(a) for a in args)):
            step(*args)

    @pl.when(core == 1)
    def _():
        alone(ready_grad, 0)
        one(early_far, DOWN, 2, 0)
        alone(ready_grad, 1)
        one(early_far, DOWN, 1)
        alone(linear, 0)
        alone(ready_act)
        alone(ready_mate, 0)
        one(start_far, DOWN, 2, 0)
        alone(linear, 1)
        alone(ready_mate, 1)
        one(start_far, DOWN, 1)
        alone(linear, 2)
        each(start_near, DOWN)

    @pl.when(core == 0)
    def _():
        alone(ready_grad, 0)
        alone(ready_grad, 1)
        alone(ready_act)
        alone(ready_mate, 0)
        one(whole_far, DOWN, 2, 0)
        alone(ready_mate, 1)
        one(whole_far, DOWN, 1)
        each(start_near, DOWN)
        alone(linear, 0)
        alone(linear, 1)
        alone(linear, 2)

    alone(linear, 3)
    alone(linear, 4)
    alone(linear, 5)
    alone(linear, 6)
    alone(linear, 7)
    each(merge1, DOWN)
    one(early_far, UP, 2, 0)
    one(early_far, UP, 1)
    one(start_own, DOWN, 2, 0)
    alone(ready_up)
    one(start_far, UP, 2, 0)
    one(start_far, UP, 1)

    @pl.when(core == 1)
    def _():
        one(start_own, DOWN, 1)
        one(start_own, UP, 2, 0, 1)
        each(start_near, UP)

    @pl.when(core == 0)
    def _():
        each(start_near, UP)
        one(start_own, DOWN, 1)
        one(start_own, UP, 2, 0, 1)

    each(merge1, UP)
    for color in colors:
        one(merged, UP, (color + 1) % 3)
        one(finish1, DOWN, color)
    each(finish1, UP)
    each(merge2, DOWN)
    each(finish2, UP)
    each(finish2, DOWN)
    each(finish3, UP)
    each(finish3, DOWN)
    alone(drain)


def local(tokens, grad_out, w_up, w_down):
    total_tokens = tokens.shape[0] * lax.axis_size("row") * lax.axis_size("col")
    factor = 1.0 / math.sqrt(total_tokens)
    anywhere = pl.BlockSpec(memory_space=pl.ANY)
    inside = pl.BlockSpec(memory_space=pltpu.VMEM)
    shape = pltpu.VMEM((64, 384), F32)
    up, down = pl.pallas_call(
        kernel,
        out_shape=(shape, shape),
        in_specs=[anywhere] * 4,
        out_specs=(inside, inside),
        scratch_shapes=[
            pltpu.VMEM((8, 2, TOK, 384), BF16),
            pltpu.VMEM((8, 2, TOK, 384), BF16),
            pltpu.VMEM((8, 768, HID), BF16),
            pltpu.VMEM((8, HID, 768), BF16),
            pltpu.VMEM((8, TOK, 384), BF16),
            pltpu.VMEM((8, TOK, 384), BF16),
            pltpu.VMEM((TOK, HID), F32),
            pltpu.VMEM((TOK, HID), F32),
            pltpu.VMEM((8, 64, TOK), BF16),
            pltpu.VMEM((8, 64, TOK), BF16),
            pltpu.VMEM((8, 64, TOK), BF16),
            pltpu.VMEM((8, 64, TOK), BF16),
            pltpu.VMEM((2, 3, 3, 16, 64, 128), BF16),
            pltpu.VMEM((2, 3, 16, 64, 128), F32),
            pltpu.VMEM((2, 3, 2, 8, 64, 128), BF16),
            pltpu.VMEM((2, 3, 2, 16, 64, 128), BF16),
            pltpu.VMEM((2, 3, 3, 4, 64, 128), BF16),
            pltpu.VMEM((2, 3, 4, 64, 128), F32),
            pltpu.VMEM((3, 2, 2, 64, 128), BF16),
            pltpu.VMEM((2, 3, 3, 4, 64, 128), BF16),
            pltpu.VMEM((2, 3, 3, 64, 128), BF16),
            pltpu.VMEM((2, 3, 64, 128), F32),
            pltpu.VMEM((2, 3, 3, 64, 128), BF16),
            pltpu.SemaphoreType.DMA((18,)),
            pltpu.SemaphoreType.DMA((4,)),
            pltpu.SemaphoreType.DMA((5,)),
            pltpu.SemaphoreType.DMA((7,)),
            pltpu.SemaphoreType.DMA((27,)),
        ],
        compiler_params=pltpu.CompilerParams(
            collective_id=0, has_side_effects=True, vmem_limit_bytes=66_000_000
        ),
    )(tokens, grad_out, w_up, w_down)
    return up.T * factor, down.T * factor


def solution(mesh):
    placed = (P(("row", "col"), None), P(("row", "col"), None), P(), P())
    return jax.shard_map(
        local,
        mesh=mesh,
        in_specs=placed,
        out_specs=(P("row", "col"), P("row", "col")),
        check_vma=False,
    )
```

```python
import math

import jax
import jax.numpy as jnp
from jax import lax
from jax.experimental import pallas as pl
from jax.experimental.pallas import tpu as pltpu
from jax.sharding import PartitionSpec as P

MESH = pl.DeviceIdType.MESH
BF16, F32 = jnp.bfloat16, jnp.float32
ROOT2, ROOT2PI = math.sqrt(2.0), math.sqrt(2.0 * math.pi)
DOWN, UP = 0, 1
TOK, WIDTH, HID = 512, 6144, 512
AHEAD = 4
FIRST = 5


def remainder(a, n):
    return lax.rem(a, jnp.int32(n))


def kernel(
    tok_hbm, grad_hbm, wup_hbm, wdn_hbm,
    up_ref, dn_ref,
    tok, grad, wup, wdn, tok_mate, grad_mate,
    pre, lin, act, act_mate, hid, hid_mate,
    part, own1, far1, got1, send2, own2, far2, got2, send3, own3, got3,
    load_sem, mate_send, mate_recv, out_sem, in_sem,
):
    row, col = lax.axis_index("row"), lax.axis_index("col")
    core = remainder(row, 2)
    at = {
        "x": (row // 8) * 2 + col // 4,
        "y": remainder(col, 4),
        "z": remainder(row // 2, 4),
    }
    mate = (row + 1 - 2 * core, col)

    def peer(axis, shift):
        to = dict(at)
        to[axis] = remainder(at[axis] + shift, 4)
        return ((to["x"] // 2) * 8 + to["z"] * 2 + core, remainder(to["x"], 2) * 4 + to["y"])

    orders = (("x", "y", "z"), ("y", "z", "x"), ("z", "x", "y"))

    barrier = pltpu.get_barrier_semaphore()
    pl.semaphore_signal(barrier, inc=1, device_id=mate, device_id_type=MESH)
    for axis in ("x", "y", "z"):
        for shift in (1, 3, 2):
            pl.semaphore_signal(barrier, inc=1, device_id=peer(axis, shift), device_id_type=MESH)

    top, deep = at["x"] // 2, at["z"]
    places = [(1 - top, 2), (top, 2), (1 - top, 0), (1 - top, 1), (1 - top, 3), (top, 0), (top, 1), (top, 3)]
    needed = [h * 4 + remainder(deep + d, 4) for h, d in places]

    def both(pair):
        return pl.ds(pl.multiple_of(pair * 768, 128), 768)

    def wide(pair, half):
        return pl.ds(pl.multiple_of(pair * 768 + half * 384, 128), 384)

    loads = []
    for pair in range(8):
        loads.append([
            pltpu.make_async_copy(wup_hbm.at[pl.ds(pair * 768, 768), :], wup.at[pair], load_sem.at[pair]),
            pltpu.make_async_copy(tok_hbm.at[:, wide(pair, 0)], tok.at[pair, 0], load_sem.at[pair]),
            pltpu.make_async_copy(tok_hbm.at[:, wide(pair, 1)], tok.at[pair, 1], load_sem.at[pair]),
        ])
    own_loads, other_loads = [], []
    for i, pair in enumerate(needed):
        own_loads.append([
            pltpu.make_async_copy(grad_hbm.at[:, wide(pair, core)], grad.at[pair, core], load_sem.at[16 if i < FIRST else 17]),
        ])
        other_loads.append([
            pltpu.make_async_copy(grad_hbm.at[:, wide(pair, 1 - core)], grad.at[pair, 1 - core], load_sem.at[8 + i]),
            pltpu.make_async_copy(wdn_hbm.at[:, both(pair)], wdn.at[pair], load_sem.at[8 + i]),
        ])
    loads += own_loads + other_loads

    def begin(group):
        for copy in loads[group]:
            copy.start()

    def finish(count, sem):
        ref = tok_mate.at[pl.ds(0, count)]
        pltpu.make_async_copy(ref, ref, sem).wait()

    def send(source, target, phase, sem, to):
        pltpu.make_async_remote_copy(
            src_ref=source, dst_ref=target, send_sem=out_sem.at[phase], recv_sem=in_sem.at[sem],
            device_id=to, device_id_type=MESH,
        ).start()

    def sem_at(bucket, color, which):
        return (bucket * 3 + color) * 4 + which

    def arrived(ref, bucket, color, which):
        pltpu.make_async_copy(ref, ref, in_sem.at[sem_at(bucket, color, which)]).wait()

    def to_mate(source, target, out, landed):
        pltpu.make_async_remote_copy(
            src_ref=source, dst_ref=target, send_sem=mate_send.at[out], recv_sem=mate_recv.at[landed],
            device_id=mate, device_id_type=MESH,
        ).start()


    def offer(i):
        to_mate(grad_hbm.at[:, wide(needed[i], 1 - core)], grad_mate.at[needed[i]], 0, 0 if i < FIRST else 1)

    for group in range(AHEAD):
        begin(group)
    with jax.named_scope("barrier"):
        pl.semaphore_wait(barrier, 10)
    def turn(target, i, value):
        target[:, :, pl.ds(i * 128, 128)] = value.astype(BF16).T.reshape(8, 64, 128)

    def turn_act(i):
        p = pre[pl.ds(i * 128, 128), :]
        turn(act, i, p * (0.5 * (1.0 + lax.erf(p / ROOT2))))

    def turn_hid(i):
        rows = pl.ds(i * 128, 128)
        turn(hid, i, lin[rows, :] * pre[rows, :])

    def in_halves(total, product, turned, source, target, out, landed):
        upper, lower = pl.ds(0, 256), pl.ds(256, 256)
        total[upper, :] += product(slice(0, 256))
        piece = product(slice(256, 512))
        turned(0)
        turned(1)
        total[lower, :] += piece
        to_mate(source.at[:, :, upper], target.at[:, :, upper], out, landed)
        turned(2)
        turned(3)
        to_mate(source.at[:, :, lower], target.at[:, :, lower], out, landed)

    for pair in range(8):
        with jax.named_scope(f"preact{pair}"):
            finish(4, load_sem.at[pair])
            begin(pair + AHEAD)
            if pair < 6:
                offer(pair)
            block = jnp.concatenate([tok[pair, 0], tok[pair, 1]], axis=1)
            if pair < 7:
                piece = jnp.dot(block, wup[pair], preferred_element_type=F32)
                pre[...] = piece if pair == 0 else pre[...] + piece
            else:
                for group in range(8 + AHEAD, 18):
                    begin(group)
                in_halves(
                    pre, lambda rows: jnp.dot(block[rows], wup[7], preferred_element_type=F32), turn_act, act, act_mate, 1, 2
                )
    offer(6)
    offer(7)
    to_mate(tok.at[:, 1 - core], tok_mate, 2, 3)

    with jax.named_scope("slope"):
        @pl.loop(0, 4)
        def _(i):
            rows = pl.ds(pl.multiple_of(i * 128, 128), 128)
            p = pre[rows, :]
            pre[rows, :] = 0.5 * (1.0 + lax.erf(p / ROOT2)) + p * (jnp.exp(-0.5 * p * p) / ROOT2PI)

    def term(left, left_mate, right, right_mate, color, shifts, sides=("own", "mate")):
        first = orders[color][0]
        lanes = pl.ds(color * 128, 128)
        places = [remainder(at[first] + shift, 4) for shift in shifts]
        if color == 0:
            (place,) = places
            pairs = [(place // 2) * 4 + z for z in range(4)]
            rows = [pl.ds(remainder(place, 2) * 4, 4)]
        elif color == 1:
            pairs = list(range(8))
            rows = [pl.ds(lo * 4 + place, 1) for place in places for lo in range(2)]
        else:
            (place,) = places
            pairs = [place, 4 + place]
            rows = [pl.ds(0, 8)]

        def lhs(ref):
            return jnp.concatenate([ref[r].reshape(r.size * 64, TOK) for r in rows], axis=0)

        a, b = [], []
        if "own" in sides:
            a.append(lhs(left))
            b.append(jnp.concatenate([right[p, core, :, lanes] for p in pairs], axis=1))
        if "mate" in sides:
            a.append(lhs(left_mate))
            b.append(jnp.concatenate([right_mate[p, :, lanes] for p in pairs], axis=1))
        out = jnp.dot(jnp.concatenate(a, axis=1), jnp.concatenate(b, axis=0), preferred_element_type=F32)
        chunks = []
        for i in range(len(shifts)):
            got = {}
            for second in range(4):
                for third in range(4):
                    if color == 0:
                        r, l = second * 64, third * 128
                    elif color == 1:
                        r, l = i * 128 + (third % 2) * 64, ((third // 2) * 4 + second) * 128
                    else:
                        r, l = ((second % 2) * 4 + third) * 64, (second // 2) * 128
                    got[second * 4 + third] = out[r:r + 64, l:l + 128]
            chunks.append(got)
        return chunks

    operands = {DOWN: (act, act_mate, grad, grad_mate), UP: (hid, hid_mate, tok, tok_mate)}
    low, high = pl.ds(0, 8), pl.ds(8, 8)
    lower, upper = pl.ds(0, 2), pl.ds(2, 2)

    def keep(bucket, color, shift, chunk):
        for i, value in chunk.items():
            if shift == 0:
                own1[bucket, color, i] = value
            else:
                part[bucket, color, shift - 1, i] = value.astype(BF16)

    def early_far(bucket, *colors):
        chunks = [term(*operands[bucket], color, (2,), ("own",))[0] for color in colors]
        for color, chunk in zip(colors, chunks):
            keep(bucket, color, 0, chunk)

    def whole_far(bucket, *colors):
        chunks = [term(*operands[bucket], color, (2,))[0] for color in colors]
        for color, chunk in zip(colors, chunks):
            keep(bucket, color, 2, chunk)
        send_far(bucket, *colors)

    def start_far(bucket, *colors):
        chunks = [term(*operands[bucket], color, (2,), ("mate",))[0] for color in colors]
        for color, chunk in zip(colors, chunks):
            keep(bucket, color, 2, {i: value + own1[bucket, color, i] for i, value in chunk.items()})
        send_far(bucket, *colors)

    def send_far(bucket, *colors):
        for color in colors:
            axis = orders[color][0]
            send(part.at[bucket, color, 1, low], far1.at[bucket, color, 0], 0, sem_at(bucket, color, 0), peer(axis, 1))
            send(part.at[bucket, color, 1, high], far1.at[bucket, color, 1], 0, sem_at(bucket, color, 0), peer(axis, 3))

    def send_next(bucket, color, half, phase=0):
        send(part.at[bucket, color, 0, half], got1.at[bucket, color, 0, half], phase, sem_at(bucket, color, 1), peer(orders[color][0], 1))

    def send_last(bucket, color, half, phase=0):
        send(part.at[bucket, color, 2, half], got1.at[bucket, color, 1, half], phase, sem_at(bucket, color, 1), peer(orders[color][0], 3))

    def start_near(bucket, color):
        if color == 1:
            chunks = term(*operands[bucket], color, (1, 3))
        else:
            chunks = [term(*operands[bucket], color, (shift,))[0] for shift in (1, 3)]
        keep(bucket, color, 1, chunks[0])
        send_next(bucket, color, high)
        keep(bucket, color, 3, chunks[1])
        send_last(bucket, color, low)

    def start_own(bucket, *colors):
        chunks = [term(*operands[bucket], color, (0,))[0] for color in colors]
        for color, chunk in zip(colors, chunks):
            keep(bucket, color, 0, chunk)

    def merge1(bucket, color):
        arrived(far1.at[bucket, color], bucket, color, 0)
        for side, shift, half, forward in ((0, 1, low, send_next), (1, 3, high, send_last)):
            part[bucket, color, shift - 1, half] = (
                part[bucket, color, shift - 1, half].astype(F32) + far1[bucket, color, side].astype(F32)
            ).astype(BF16)
            forward(bucket, color, half, 1 if bucket == DOWN else 2 + color)

    def merged(bucket, color):
        pltpu.make_async_copy(part.at[bucket, color, 0], part.at[bucket, color, 0], out_sem.at[2 + color]).wait()

    def total1(bucket, color, shift):
        place = pl.ds(remainder(at[orders[color][1]] + shift, 4) * 4, 4)
        return (
            own1[bucket, color, place]
            + got1[bucket, color, 0, place].astype(F32)
            + got1[bucket, color, 1, place].astype(F32)
        )

    def send_second(bucket, color, source, target, sem, shift):
        send(source, target, 5, sem, peer(orders[color][1], shift))

    def finish1(bucket, color):
        arrived(got1.at[bucket, color], bucket, color, 1)
        sem = sem_at(bucket, color, 2)
        for shift in (2, 1, 3):
            out = send2.at[bucket, color, shift - 1]
            send2[bucket, color, shift - 1] = total1(bucket, color, shift).astype(BF16)
            if bucket == UP:
                send_second(bucket, color, out, got2.at[bucket, color, shift - 1], sem, shift)
            elif shift == 2:
                send_second(bucket, color, out.at[lower], far2.at[color, 0], 24 + color, 1)
                send_second(bucket, color, out.at[upper], far2.at[color, 1], 24 + color, 3)
            elif shift == 1:
                send_second(bucket, color, out.at[upper], got2.at[bucket, color, 0, upper], sem, 1)
            else:
                send_second(bucket, color, out.at[lower], got2.at[bucket, color, 1, lower], sem, 3)
        own2[bucket, color] = total1(bucket, color, 0)

    def merge2(bucket, color):
        pltpu.make_async_copy(far2.at[color], far2.at[color], in_sem.at[24 + color]).wait()
        for side, shift, half in ((0, 1, lower), (1, 3, upper)):
            send2[bucket, color, shift - 1, half] = (
                send2[bucket, color, shift - 1, half].astype(F32) + far2[color, side].astype(F32)
            ).astype(BF16)
            send_second(
                bucket, color, send2.at[bucket, color, shift - 1, half], got2.at[bucket, color, side, half],
                sem_at(bucket, color, 2), shift,
            )

    def finish2(bucket, color):
        axis = orders[color][2]
        count = 2 if bucket == DOWN else 3
        arrived(got2.at[bucket, color, pl.ds(0, count)], bucket, color, 2)

        def total(place):
            value = own2[bucket, color, place]
            for i in range(count):
                value = value + got2[bucket, color, i, place].astype(F32)
            return value

        for shift in (2, 1, 3):
            send3[bucket, color, shift - 1] = total(remainder(at[axis] + shift, 4)).astype(BF16)
            send(send3.at[bucket, color, shift - 1], got3.at[bucket, color, shift - 1], 6, sem_at(bucket, color, 3), peer(axis, shift))
        own3[bucket, color] = total(at[axis])

    def finish3(bucket, color):
        arrived(got3.at[bucket, color], bucket, color, 3)
        value = own3[bucket, color]
        for i in range(3):
            value = value + got3[bucket, color, i].astype(F32)
        out = dn_ref if bucket == DOWN else up_ref
        out[:, pl.ds(color * 128, 128)] = value

    colors = (2, 0, 1)

    def linear(i):
        pair = needed[i]
        finish(3, load_sem.at[8 + i])
        block = jnp.concatenate([grad[pair, 0], grad[pair, 1]], axis=1)

        def product(rows):
            return lax.dot_general(block[rows], wdn[pair], (((1,), (1,)), ((), ())), preferred_element_type=F32)

        if i == 7:
            in_halves(lin, product, turn_hid, hid, hid_mate, 3, 4)
        else:
            piece = product(slice(0, 512))
            lin[...] = piece if i == 0 else lin[...] + piece

    def ready_grad(which):
        finish((FIRST, 8 - FIRST)[which], load_sem.at[16 + which])

    def ready_mate(which):
        finish((FIRST, 8 - FIRST)[which], mate_recv.at[which])

    def ready_act():
        pltpu.make_async_copy(act_mate, act_mate, mate_recv.at[2]).wait()
        for group in range(18, 24):
            begin(group)

    def ready_up():
        pltpu.make_async_copy(tok_mate, tok_mate, mate_recv.at[3]).wait()
        pltpu.make_async_copy(hid_mate, hid_mate, mate_recv.at[4]).wait()

    def drain():
        for i, ref in enumerate((grad_mate, act, tok_mate, hid)):
            pltpu.make_async_copy(ref, ref, mate_send.at[i]).wait()
        for i, ref in ((0, part.at[:, :, pl.ds(0, 2)]), (1, part.at[DOWN, :, 0]), (5, send2), (6, send3)):
            pltpu.make_async_copy(ref, ref, out_sem.at[i]).wait()

    def one(step, bucket, *colors):
        with jax.named_scope(f"{step.__name__}_{'DU'[bucket]}" + "".join(map(str, colors))):
            step(bucket, *colors)

    def each(step, bucket):
        for color in colors:
            one(step, bucket, color)

    def alone(step, *args):
        with jax.named_scope(step.__name__ + "_".join(str(a) for a in args)):
            step(*args)

    @pl.when(core == 1)
    def _():
        alone(ready_grad, 0)
        one(early_far, DOWN, 2, 0)
        alone(ready_grad, 1)
        one(early_far, DOWN, 1)
        alone(linear, 0)
        alone(ready_act)
        alone(ready_mate, 0)
        one(start_far, DOWN, 2, 0)
        alone(linear, 1)
        alone(ready_mate, 1)
        one(start_far, DOWN, 1)
        alone(linear, 2)
        each(start_near, DOWN)

    @pl.when(core == 0)
    def _():
        alone(ready_grad, 0)
        alone(ready_act)
        alone(ready_mate, 0)
        one(whole_far, DOWN, 2, 0)
        alone(linear, 0)
        alone(ready_grad, 1)
        alone(ready_mate, 1)
        one(whole_far, DOWN, 1)
        each(start_near, DOWN)
        alone(linear, 1)
        alone(linear, 2)

    alone(linear, 3)
    alone(linear, 4)
    alone(linear, 5)
    alone(linear, 6)
    alone(linear, 7)
    each(merge1, DOWN)
    one(early_far, UP, 2, 0)
    one(early_far, UP, 1)
    one(start_own, DOWN, 2, 0)
    alone(ready_up)
    one(start_far, UP, 2, 0)
    one(start_far, UP, 1)

    @pl.when(core == 1)
    def _():
        one(start_own, DOWN, 1)
        one(start_own, UP, 2, 0, 1)
        each(start_near, UP)

    @pl.when(core == 0)
    def _():
        each(start_near, UP)
        one(start_own, DOWN, 1)
        one(start_own, UP, 2, 0, 1)

    each(merge1, UP)
    @pl.when(core == 1)
    def _():
        for color in colors:
            one(merged, UP, (color + 1) % 3)
            one(finish1, DOWN, color)

    @pl.when(core == 0)
    def _():
        each(finish1, DOWN)
        for color in colors:
            one(merged, UP, color)

    each(finish1, UP)
    each(merge2, DOWN)
    each(finish2, UP)
    each(finish2, DOWN)
    each(finish3, UP)
    each(finish3, DOWN)
    alone(drain)


def local(tokens, grad_out, w_up, w_down):
    total_tokens = tokens.shape[0] * lax.axis_size("row") * lax.axis_size("col")
    factor = 1.0 / math.sqrt(total_tokens)
    anywhere = pl.BlockSpec(memory_space=pl.ANY)
    inside = pl.BlockSpec(memory_space=pltpu.VMEM)
    shape = pltpu.VMEM((64, 384), F32)
    up, down = pl.pallas_call(
        kernel,
        out_shape=(shape, shape),
        in_specs=[anywhere] * 4,
        out_specs=(inside, inside),
        scratch_shapes=[
            pltpu.VMEM((8, 2, TOK, 384), BF16),
            pltpu.VMEM((8, 2, TOK, 384), BF16),
            pltpu.VMEM((8, 768, HID), BF16),
            pltpu.VMEM((8, HID, 768), BF16),
            pltpu.VMEM((8, TOK, 384), BF16),
            pltpu.VMEM((8, TOK, 384), BF16),
            pltpu.VMEM((TOK, HID), F32),
            pltpu.VMEM((TOK, HID), F32),
            pltpu.VMEM((8, 64, TOK), BF16),
            pltpu.VMEM((8, 64, TOK), BF16),
            pltpu.VMEM((8, 64, TOK), BF16),
            pltpu.VMEM((8, 64, TOK), BF16),
            pltpu.VMEM((2, 3, 3, 16, 64, 128), BF16),
            pltpu.VMEM((2, 3, 16, 64, 128), F32),
            pltpu.VMEM((2, 3, 2, 8, 64, 128), BF16),
            pltpu.VMEM((2, 3, 2, 16, 64, 128), BF16),
            pltpu.VMEM((2, 3, 3, 4, 64, 128), BF16),
            pltpu.VMEM((2, 3, 4, 64, 128), F32),
            pltpu.VMEM((3, 2, 2, 64, 128), BF16),
            pltpu.VMEM((2, 3, 3, 4, 64, 128), BF16),
            pltpu.VMEM((2, 3, 3, 64, 128), BF16),
            pltpu.VMEM((2, 3, 64, 128), F32),
            pltpu.VMEM((2, 3, 3, 64, 128), BF16),
            pltpu.SemaphoreType.DMA((18,)),
            pltpu.SemaphoreType.DMA((4,)),
            pltpu.SemaphoreType.DMA((5,)),
            pltpu.SemaphoreType.DMA((7,)),
            pltpu.SemaphoreType.DMA((27,)),
        ],
        compiler_params=pltpu.CompilerParams(
            collective_id=0, has_side_effects=True, vmem_limit_bytes=66_000_000
        ),
    )(tokens, grad_out, w_up, w_down)
    return up.T * factor, down.T * factor


def solution(mesh):
    placed = (P(("row", "col"), None), P(("row", "col"), None), P(), P())
    return jax.shard_map(
        local,
        mesh=mesh,
        in_specs=placed,
        out_specs=(P("row", "col"), P("row", "col")),
        check_vma=False,
    )
```
